256 devices in a mesh: pair: 16 (over x_lo, z), aux: 16 (over y, x_hi, core).
Axes of the slice: x: 4 (x_hi: 2, x_lo: 2; x = x_hi * 2 + x_lo), y: 4, z: 8, core: 2. Of those that a mesh axis runs over, the one named last changes fastest.
Arguments:
- panels: bfloat16 [32, 120, 36864], P('pair', None, 'aux'), may hold values from -1 to 1
- amplitudes: bfloat16 [32, 2, 120, 120], P('pair'), may hold values from -0.5 to 0.5
- drive: float32 [32, 2, 14400], P('pair', None, 'aux'), may hold values from -6 to 6
- pno_energy: float32 [32, 120], P('pair'), may hold values from 1 to 3
- occ_energy: float32 [64], replicated, may hold values from -2 to -0.5
- frequency: float32 [1], replicated, may hold values from 0.2 to 2
- pair_lmo: int32 [32, 2], replicated, may hold values from 0 to 63
- neighbours: int32 [32, 8], P('pair'), may hold values from 0 to 31
- pno_ranks: int32 [32], P('pair'), may hold values from 60 to 120
- fock_off: float32 [64, 64], replicated, may hold values from -1.8 to 1.8
Outputs:
- residual: float32 [32, 2, 14400], P('pair', None, 'aux')
The draws below stay inside these ranges and needn't reach their ends.
Inputs may be any that keep to these rules, and one draw needn't show every extreme that they name: `neighbours`: neighbour pairs; a pair may be listed more than once and may list itself. `pno_ranks`: rows of a pair's panel from its rank on are padding.
All inputs are finite; a program needn't handle non-finite values.
Results may differ from the reference program's by a relative error of at most 0.0033.
Values may be sent and summed in bfloat16 or wider, within the bound.
A program may use at most 128 MiB of HBM per device.

```python
import jax
import jax.numpy as jnp
from jax import lax

R = 120
AUX_DEV = 2304
AUX = 36864
PAIRS = 32
NBR = 8
NLMO = 64
RR = 14400
N_AUX = 16


def plant(values, rng, least, high):
    longest = values.shape.index(max(values.shape))
    spots = []
    for shift in (0, 1):
        where = [jax.random.randint(jax.random.fold_in(rng, axis), (), 0, length) for axis, length in enumerate(values.shape)]
        where[longest] = (where[longest] + shift) % values.shape[longest]
        spots.append(tuple(where))
    return values.at[spots[0]].set(least).at[spots[1]].set(high)


def levels(own_key, shape, pieces, least, largest):
    def one(axis_at, shards_of):
        draws = jax.random.uniform(jax.random.fold_in(jax.random.fold_in(own_key, 6), axis_at), (shards_of,), jnp.float32, least / len(pieces), largest / len(pieces))
        return jnp.repeat(jnp.exp(draws), shape[axis_at] // shards_of).reshape((-1,) + (1,) * (len(shape) - axis_at - 1))

    loudness = one(*pieces[0])
    for cut in pieces[1:]:
        loudness = loudness * one(*cut)
    return loudness


def bell_draw(rng, dims, width, reach, split=(), kind=jnp.bfloat16):
    entries = jax.random.normal(rng, dims, jnp.float32) * width
    if len(split) > 0:
        entries = levels(rng, dims, split, -0.22, 0.18) * entries
    return jnp.clip(entries, min=-reach, max=reach).astype(kind)


def setup_inputs(seed: int = 0) -> dict:
    splits = jax.random.split(jax.random.key(seed), 11)
    return {
        "panels": bell_draw(splits[0], (PAIRS, R, AUX), (AUX ** -0.25), 1.0, ((0, 16), (2, 16))),
        "amplitudes": bell_draw(splits[1], (PAIRS, 2, R, R), R ** -0.5, 0.5, ((0, 16),)),
        "drive": bell_draw(splits[2], (PAIRS, 2, RR), 1.0, 6.0, ((0, 16), (2, 16)), jnp.float32),
        "pno_energy": jnp.clip(1.0 + 2.0 * jax.random.uniform(splits[3], (PAIRS, R), jnp.float32) ** levels(splits[3], (PAIRS, R), ((0, 16),), -0.2, 0.2), 1.0, 3.0),
        "occ_energy": jnp.clip(jax.random.uniform(splits[4], (NLMO,), jnp.float32, -2.0, -0.5), -2.0, -0.5),
        "frequency": jnp.clip(jax.random.uniform(splits[5], (1,), jnp.float32, 0.2, 2.0), 0.2, 2.0),
        "pair_lmo": plant(jax.random.randint(splits[6], (PAIRS, 2), 0, NLMO), jax.random.fold_in(splits[6], 1), 0, NLMO - 1).astype(jnp.int32),
        "neighbours": plant(jax.random.randint(splits[7], (PAIRS, NBR), 0, PAIRS), jax.random.fold_in(splits[7], 1), 0, PAIRS - 1).astype(jnp.int32),
        "pno_ranks": plant(jax.random.randint(splits[8], (PAIRS,), R // 2, R + 1), jax.random.fold_in(splits[8], 1), R // 2, R).astype(jnp.int32),
        "fock_off": bell_draw(splits[9], (NLMO, NLMO), 0.3, 1.8, (), jnp.float32),
    }


def reference(panels, amplitudes, drive, pno_energy, occ_energy, frequency, pair_lmo, neighbours, pno_ranks, fock_off):
    rows_index = jnp.arange(R, dtype=jnp.int32)
    keep_rows = rows_index[None, :] < pno_ranks[:, None]
    masked = jnp.where(keep_rows[:, :, None], panels, jnp.zeros_like(panels))
    near_lmo = pair_lmo[neighbours]
    values = fock_off[pair_lmo[:, 0][:, None], near_lmo[:, :, 0]] + fock_off[pair_lmo[:, 1][:, None], near_lmo[:, :, 1]]
    onehot = (neighbours[:, :, None] == jnp.arange(PAIRS, dtype=jnp.int32)[None, None, :]).astype(jnp.float32)
    weights = jnp.sum(values[:, :, None] * onehot, axis=1).astype(jnp.bfloat16)
    weights_wide = weights.astype(jnp.float32)
    matrices = jnp.transpose(amplitudes, (0, 2, 1, 3)).reshape(PAIRS, R, 2 * R).astype(jnp.float32)

    def block_step(running_sum, block_index):
        start_col = (block_index * AUX_DEV).astype(jnp.int32)
        slab = lax.dynamic_slice_in_dim(masked, start_col, AUX_DEV, 2).astype(jnp.float32)
        projected = jnp.einsum('nra,nrc->nac', slab, matrices, precision=lax.Precision.HIGHEST).astype(jnp.bfloat16)
        projected = lax.optimization_barrier(projected).astype(jnp.float32)
        collected = jnp.einsum('pn,nac->pac', weights_wide, projected, precision=lax.Precision.HIGHEST).astype(jnp.bfloat16)
        collected = lax.optimization_barrier(collected).astype(jnp.float32)
        running_sum = running_sum + jnp.einsum('pra,pac->prc', slab, collected, precision=lax.Precision.HIGHEST)
        return running_sum, None

    start_sum = jnp.zeros((PAIRS, R, 2 * R), jnp.float32)
    coupled, unused_out = lax.scan(block_step, start_sum, jnp.arange(N_AUX, dtype=jnp.int32))
    coupled = jnp.transpose(coupled.reshape(PAIRS, R, 2, R), (0, 2, 1, 3))
    occ_pair = occ_energy[pair_lmo[:, 0]] + occ_energy[pair_lmo[:, 1]]
    shift = pno_energy[:, :, None] + pno_energy[:, None, :] - occ_pair[:, None, None]
    signs = jnp.array([1.0, -1.0], jnp.float32)
    factor = shift[:, None, :, :] - signs[None, :, None, None] * frequency[0]
    diagonal_term = factor * amplitudes.astype(jnp.float32)
    return drive + diagonal_term.reshape(PAIRS, 2, R * R) + coupled.reshape(PAIRS, 2, R * R)
```

```python
import math

import jax
import jax.numpy as jnp
from jax import lax
from jax.sharding import PartitionSpec as P


def cut_along(shard, dim, length):
    before, after = (shard.shape[:dim], shard.shape[dim + 1 :])
    return jnp.moveaxis(shard.reshape(*before, length, -1, *after), dim, 0)


def sent_and_summed(shard, axis, dim):
    length = lax.axis_size(axis)
    blocks = lax.all_to_all(cut_along(shard, dim, length), axis, 0, 0, tiled=True)
    return jnp.sum(blocks.astype(jnp.float32), axis=0)


def pair_weights(pair_lmo, neighbours, fock_off, first_pair):
    local_pairs = neighbours.shape[0]
    total_pairs = pair_lmo.shape[0]
    lmo_count = fock_off.shape[0]
    lmo_ids = jnp.arange(lmo_count, dtype=jnp.int32)
    own_lmo = lax.dynamic_slice_in_dim(pair_lmo, first_pair, local_pairs, 0)
    own_table = (own_lmo[:, :, None] == lmo_ids[None, None, :]).astype(jnp.float32)
    lmo_table = (pair_lmo[:, :, None] == lmo_ids[None, None, :]).astype(jnp.float32)
    pair_ids = jnp.arange(total_pairs, dtype=jnp.int32)
    onehot = (neighbours[:, :, None] == pair_ids[None, None, :]).astype(jnp.float32)
    fock_rows = jnp.einsum("psl,lm->psm", own_table, fock_off, precision=lax.Precision.HIGHEST)
    near_table = jnp.einsum("pkn,nsl->pksl", onehot, lmo_table)
    values = jnp.sum(fock_rows[:, None, :, :] * near_table, axis=(2, 3))
    weights = jnp.sum(values[:, :, None] * onehot, axis=1).astype(jnp.bfloat16)
    return (weights, own_table)


def spread_panels(masked):
    local_pairs, rank_dim, aux_width = masked.shape
    length = lax.axis_size("pair")
    blocks = cut_along(masked, 2, length)
    swapped = lax.all_to_all(blocks, "pair", 0, 0, tiled=True)
    return swapped.reshape(length * local_pairs, rank_dim, aux_width // length)


def body(
    panels,
    amplitudes,
    drive,
    pno_energy,
    occ_energy,
    frequency,
    pair_lmo,
    neighbours,
    pno_ranks,
    fock_off,
):
    local_pairs, rank_dim, aux_width = panels.shape
    first_pair = lax.axis_index("pair") * local_pairs
    rows_index = jnp.arange(rank_dim, dtype=jnp.int32)
    keep_rows = rows_index[None, :] < pno_ranks[:, None]
    masked = jnp.where(keep_rows[:, :, None], panels, jnp.zeros_like(panels))
    weights, own_table = pair_weights(pair_lmo, neighbours, fock_off, first_pair)
    all_weights = lax.all_gather(weights, "pair", axis=0, tiled=True)
    all_amps = lax.all_gather(amplitudes, "pair", axis=0, tiled=True)
    slices = spread_panels(masked)
    projected = jnp.einsum(
        "naq,nsac->nsqc", slices, all_amps, preferred_element_type=jnp.float32
    ).astype(jnp.bfloat16)
    collected = jnp.einsum(
        "pn,nsqc->psqc", all_weights, projected, preferred_element_type=jnp.float32
    ).astype(jnp.bfloat16)
    coupled = jnp.einsum(
        "paq,psqc->psac", slices, collected, preferred_element_type=jnp.float32
    ).astype(jnp.bfloat16)
    coupled = coupled.reshape(coupled.shape[0], 2, rank_dim * rank_dim)
    over_aux = sent_and_summed(coupled, "aux", 2).astype(jnp.bfloat16)
    coupled_share = sent_and_summed(over_aux, "pair", 0)
    share_width = drive.shape[2]
    share_start = lax.axis_index("aux") * share_width
    occ_pair = jnp.sum(own_table * occ_energy[None, None, :], axis=(1, 2))
    shift = pno_energy[:, :, None] + pno_energy[:, None, :] - occ_pair[:, None, None]
    shift_flat = lax.dynamic_slice_in_dim(
        shift.reshape(local_pairs, rank_dim * rank_dim), share_start, share_width, 1
    )
    signs = jnp.array([1.0, -1.0], jnp.float32)
    factor = shift_flat[:, None, :] - signs[None, :, None] * frequency[0]
    amp_flat = amplitudes.reshape(local_pairs, 2, rank_dim * rank_dim)
    amp_share = lax.dynamic_slice_in_dim(amp_flat, share_start, share_width, 2).astype(jnp.float32)
    return drive + factor * amp_share + coupled_share


def solution(mesh):
    placed = (
        P("pair", None, "aux"),
        P("pair", None, None, None),
        P("pair", None, "aux"),
        P("pair", None),
        P(),
        P(),
        P(),
        P("pair", None),
        P("pair"),
        P(),
    )
    return jax.shard_map(
        body, mesh=mesh, in_specs=placed, out_specs=P("pair", None, "aux"), check_vma=False
    )
```

```python
import jax
import jax.numpy as jnp
from jax import lax
from jax.experimental import pallas as pl
from jax.experimental.pallas import tpu as pltpu
from jax.sharding import PartitionSpec as P

MESH = pl.DeviceIdType.MESH

PAIR_STEPS = [(1, 0)] + [(dx, dz) for dz in (1, 7, 2, 6, 3, 5, 4) for dx in (0, 1)]
CHIP_STEPS = [(0, 1), (1, 0), (3, 0), (1, 1), (3, 1), (2, 0), (2, 1)]
GROUP = 4


def kernel(
    mt_ref,
    amp_ref,
    nbr_ref,
    wgt_ref,
    out_ref,
    mbuf,
    abuf,
    nbuf,
    wbuf,
    nsm,
    wsm,
    proj,
    mtr,
    coll,
    sbuf,
    rbuf,
    tbuf,
    ubuf,
    fin,
    m_send,
    m_recv,
    f_send,
    f_recv,
    a_send,
    a_recv,
    g_send,
    g_recv,
    c_send,
    c_recv,
    n_send,
    n_recv,
    w_send,
    w_recv,
    s_sem,
    r_send,
    r_recv,
    u_send,
    u_recv,
    x_send,
    x_recv,
):
    pair = lax.axis_index("pair")
    aux = lax.axis_index("aux")
    xlo, z = pair // 8, lax.rem(pair, 8)
    chip, core = aux // 2, lax.rem(aux, 2)
    y, xhi = chip // 2, lax.rem(chip, 2)
    other = 1 - core
    partner = (pair, chip * 2 + other)

    def pair_to(step):
        dx, dz = step
        return lax.rem(xlo + dx, 2) * 8 + lax.rem(z + dz, 8)

    def pair_from(step):
        dx, dz = step
        return lax.rem(xlo + dx, 2) * 8 + lax.rem(z + 8 - dz, 8)

    def chip_to(step):
        dy, dx = step
        return lax.rem(y + dy, 4) * 2 + lax.rem(xhi + dx, 2)

    def chip_from(step):
        dy, dx = step
        return lax.rem(y + 4 - dy, 4) * 2 + lax.rem(xhi + dx, 2)

    barrier = pltpu.get_barrier_semaphore()
    for step in PAIR_STEPS:
        pl.semaphore_signal(barrier, inc=1, device_id=(pair_from(step), aux), device_id_type=MESH)
    for step in CHIP_STEPS:
        pl.semaphore_signal(
            barrier, inc=1, device_id=(pair, chip_from(step) * 2 + core), device_id_type=MESH
        )
    pl.semaphore_signal(barrier, inc=1, device_id=partner, device_id_type=MESH)

    def remote(src, dst, send, recv, target):
        return pltpu.make_async_remote_copy(
            src_ref=src,
            dst_ref=dst,
            send_sem=send,
            recv_sem=recv,
            device_id=target,
            device_id_type=MESH,
        )

    def m_rows(p):
        return mt_ref.at[:, pl.ds(pl.multiple_of(p * 144, 16), 144), :]

    abuf[chip, core, pair] = amp_ref[...]
    nbuf[pair] = nbr_ref[...]
    wbuf[pair] = wgt_ref[...]
    pl.semaphore_wait(barrier, 23)

    for i, step in enumerate(PAIR_STEPS):
        to = (pair_to(step), aux)
        remote(amp_ref, abuf.at[chip, core, pair], a_send.at[i], a_recv.at[i], to).start()
        remote(nbr_ref, nbuf.at[pair], n_send.at[i], n_recv.at[i], to).start()
        remote(wgt_ref, wbuf.at[pair], w_send.at[i], w_recv.at[i], to).start()
    for i, step in enumerate(PAIR_STEPS):
        p = pair_to(step)
        remote(m_rows(p), mbuf.at[pair, core], m_send.at[i], m_recv.at[i], (p, aux)).start()
    own_to_partner = remote(
        m_rows(pair), mbuf.at[pair, core], f_send.at[15], f_recv.at[15], partner
    )
    own_to_partner.start()
    mbuf[pair, core] = mt_ref[:, pl.ds(pl.multiple_of(pair * 144, 16), 144), :]

    for i, step in enumerate(PAIR_STEPS):
        p = pair_from(step)
        remote(amp_ref, abuf.at[chip, core, p], a_send.at[i], a_recv.at[i], (p, aux)).wait_recv()
    for i, step in enumerate(CHIP_STEPS):
        to = (pair, chip_to(step) * 2 + core)
        remote(
            abuf.at[chip, core], abuf.at[chip, core], g_send.at[i], g_recv.at[i], to
        ).start()
    remote(
        abuf.at[chip, core], abuf.at[chip, core], c_send.at[7], c_recv.at[7], partner
    ).start()

    for i, step in enumerate(PAIR_STEPS):
        p = pair_from(step)
        remote(nbr_ref, nbuf.at[p], n_send.at[i], n_recv.at[i], (p, aux)).wait_recv()
        remote(wgt_ref, wbuf.at[p], w_send.at[i], w_recv.at[i], (p, aux)).wait_recv()
    to_nsm = pltpu.make_async_copy(nbuf, nsm, s_sem.at[0])
    to_wsm = pltpu.make_async_copy(wbuf, wsm, s_sem.at[1])
    to_nsm.start()
    to_wsm.start()
    to_nsm.wait()
    to_wsm.wait()

    def relay_block(i):
        step = PAIR_STEPS[i]
        p = pair_from(step)
        remote(m_rows(p), mbuf.at[p, core], m_send.at[i], m_recv.at[i], (p, aux)).wait_recv()
        remote(
            mbuf.at[p, core], mbuf.at[p, core], f_send.at[i], f_recv.at[i], partner
        ).start()

    def relayed(i):
        p = pair if i == 15 else pair_from(PAIR_STEPS[i])
        remote(
            mbuf.at[p, other], mbuf.at[p, other], f_send.at[i], f_recv.at[i], partner
        ).wait_recv()
        for h in range(2):
            mtr[p, h] = mbuf[p, h, core].T
        return p

    def project(p):
        for c in range(2):
            matrix = abuf[:, c, p].reshape(128, 256)
            for h in range(2):
                proj[2 * p + c, h] = jnp.dot(
                    mbuf[p, h, c], matrix, preferred_element_type=jnp.float32
                ).astype(jnp.bfloat16)

    early = 9
    relayed(15)
    for i in range(early):
        relay_block(i)
        if i:
            relayed(i - 1)
    for i, step in enumerate(CHIP_STEPS):
        g = chip_from(step)
        remote(
            abuf.at[g, core], abuf.at[g, core], g_send.at[i], g_recv.at[i], (pair, g * 2 + core)
        ).wait_recv()
        remote(abuf.at[g, core], abuf.at[g, core], c_send.at[i], c_recv.at[i], partner).start()
    relayed(early - 1)
    relay_block(early)
    for i in range(8):
        g = chip if i == 7 else chip_from(CHIP_STEPS[i])
        remote(
            abuf.at[g, other], abuf.at[g, other], c_send.at[i], c_recv.at[i], partner
        ).wait_recv()
    project(pair)
    for i in range(early):
        project(pair_from(PAIR_STEPS[i]))
    for i in range(early, 15):
        if i + 1 < 15:
            relay_block(i + 1)
        project(relayed(i))

    def one_pair(p):
        for h in range(2):
            total = jnp.zeros((144, 256), jnp.float32)
            for k in range(8):
                n = nsm[p, 0, core * 8 + k]
                w = wsm[p, 0, core * 8 + k]
                total = total + w * proj[n, h].astype(jnp.float32)
            coll[h] = total.astype(jnp.bfloat16)
        closed = jnp.dot(mtr[p, 0], coll[0], preferred_element_type=jnp.float32)
        closed = closed + jnp.dot(mtr[p, 1], coll[1], preferred_element_type=jnp.float32)
        sbuf[:, p] = closed.astype(jnp.bfloat16).reshape(8, 16, 256)

    def part(q):
        return pl.ds(q * GROUP, GROUP)

    groups = 16 // GROUP
    for q in range(groups):
        lax.fori_loop(q * GROUP, (q + 1) * GROUP, lambda p, x: (one_pair(p), x)[1], 0)
        for i, step in enumerate(CHIP_STEPS):
            g = chip_to(step)
            remote(
                sbuf.at[g, part(q)],
                rbuf.at[i, part(q)],
                r_send.at[q, i],
                r_recv.at[q, i],
                (pair, g * 2 + core),
            ).start()
    for q in range(groups):
        for i, step in enumerate(CHIP_STEPS):
            g = chip_from(step)
            remote(
                sbuf.at[g, part(q)],
                rbuf.at[i, part(q)],
                r_send.at[q, i],
                r_recv.at[q, i],
                (pair, g * 2 + core),
            ).wait_recv()
        total = sbuf[chip, part(q)].astype(jnp.float32)
        for i in range(7):
            total = total + rbuf[i, part(q)].astype(jnp.float32)
        tbuf[part(q)] = total.astype(jnp.bfloat16)
        for j in range(GROUP):
            p = q * GROUP + j
            slot = lax.rem(xlo + p // 8, 2) * 8 + lax.rem(p % 8 - z + 8, 8)

            @pl.when(p != pair)
            def _():
                remote(
                    tbuf.at[p], ubuf.at[slot], u_send.at[slot], u_recv.at[slot], (p, aux)
                ).start()

    total = tbuf[pair].astype(jnp.float32)
    for slot in range(1, 16):
        p = pair_from((slot // 8, slot % 8))
        remote(
            tbuf.at[p], ubuf.at[slot], u_send.at[slot], u_recv.at[slot], (p, aux)
        ).wait_recv()
        total = total + ubuf[slot].astype(jnp.float32)
    fin[core] = total
    swap = remote(fin.at[core], fin.at[core], x_send, x_recv, partner)
    swap.start()
    out_ref[core] = total
    remote(fin.at[other], fin.at[other], x_send, x_recv, partner).wait_recv()
    out_ref[other] = fin[other]

    for i, step in enumerate(PAIR_STEPS):
        to = (pair_to(step), aux)
        remote(amp_ref, abuf.at[chip, core, pair], a_send.at[i], a_recv.at[i], to).wait_send()
        remote(nbr_ref, nbuf.at[pair], n_send.at[i], n_recv.at[i], to).wait_send()
        remote(wgt_ref, wbuf.at[pair], w_send.at[i], w_recv.at[i], to).wait_send()
        p = pair_to(step)
        remote(m_rows(p), mbuf.at[pair, core], m_send.at[i], m_recv.at[i], to).wait_send()
        p = pair_from(step)
        remote(
            mbuf.at[p, core], mbuf.at[p, core], f_send.at[i], f_recv.at[i], partner
        ).wait_send()
    own_to_partner.wait_send()
    for i, step in enumerate(CHIP_STEPS):
        to = (pair, chip_to(step) * 2 + core)
        remote(
            abuf.at[chip, core], abuf.at[chip, core], g_send.at[i], g_recv.at[i], to
        ).wait_send()
        for q in range(groups):
            remote(
                sbuf.at[chip, part(q)], rbuf.at[i, part(q)], r_send.at[q, i], r_recv.at[q, i], to
            ).wait_send()
        g = chip_from(step)
        remote(abuf.at[g, core], abuf.at[g, core], c_send.at[i], c_recv.at[i], partner).wait_send()
    remote(
        abuf.at[chip, core], abuf.at[chip, core], c_send.at[7], c_recv.at[7], partner
    ).wait_send()
    for slot in range(1, 16):
        p = pair_to((slot // 8, slot % 8))
        remote(
            tbuf.at[p], ubuf.at[slot], u_send.at[slot], u_recv.at[slot], (p, aux)
        ).wait_send()
    swap.wait_send()


def coupled_rows(mt, amp_piece, nbr_row, wgt_row):
    bf16, f32, i32 = jnp.bfloat16, jnp.float32, jnp.int32
    dma = pltpu.SemaphoreType.DMA
    groups = 16 // GROUP
    return pl.pallas_call(
        kernel,
        out_shape=jax.ShapeDtypeStruct((2, 16, 256), f32),
        in_specs=[pl.BlockSpec(memory_space=pltpu.VMEM)] * 4,
        out_specs=pl.BlockSpec(memory_space=pltpu.VMEM),
        scratch_shapes=[
            pltpu.VMEM((16, 2, 2, 144, 128), bf16),
            pltpu.VMEM((8, 2, 16, 16, 256), bf16),
            pltpu.VMEM((16, 1, 128), i32),
            pltpu.VMEM((16, 1, 128), f32),
            pltpu.SMEM((16, 1, 128), i32),
            pltpu.SMEM((16, 1, 128), f32),
            pltpu.VMEM((32, 2, 144, 256), bf16),
            pltpu.VMEM((16, 2, 128, 144), bf16),
            pltpu.VMEM((2, 144, 256), bf16),
            pltpu.VMEM((8, 16, 16, 256), bf16),
            pltpu.VMEM((7, 16, 16, 256), bf16),
            pltpu.VMEM((16, 16, 256), bf16),
            pltpu.VMEM((16, 16, 256), bf16),
            pltpu.VMEM((2, 16, 256), f32),
            dma((15,)),
            dma((15,)),
            dma((16,)),
            dma((16,)),
            dma((15,)),
            dma((15,)),
            dma((7,)),
            dma((7,)),
            dma((8,)),
            dma((8,)),
            dma((15,)),
            dma((15,)),
            dma((15,)),
            dma((15,)),
            dma((2,)),
            dma((groups, 7)),
            dma((groups, 7)),
            dma((16,)),
            dma((16,)),
            dma,
            dma,
        ],
        compiler_params=pltpu.CompilerParams(
            collective_id=0, has_side_effects=True, vmem_limit_bytes=56 << 20
        ),
        name="coupled_rows",
    )(mt, amp_piece, nbr_row, wgt_row)


def slot_weights(pair_lmo, neighbours, fock_off, first_pair):
    local_pairs, slots = neighbours.shape
    total_pairs = pair_lmo.shape[0]
    lmo_count = fock_off.shape[0]
    lmo_ids = jnp.arange(lmo_count, dtype=jnp.int32)
    own_lmo = lax.dynamic_slice_in_dim(pair_lmo, first_pair, local_pairs, 0)
    own_table = (own_lmo[:, :, None] == lmo_ids[None, None, :]).astype(jnp.float32)
    lmo_table = (pair_lmo[:, :, None] == lmo_ids[None, None, :]).astype(jnp.float32)
    pair_ids = jnp.arange(total_pairs, dtype=jnp.int32)
    onehot = (neighbours[:, :, None] == pair_ids[None, None, :]).astype(jnp.float32)
    fock_rows = jnp.einsum("psl,lm->psm", own_table, fock_off, precision=lax.Precision.HIGHEST)
    near_table = jnp.einsum("pkn,nsl->pksl", onehot, lmo_table)
    values = jnp.sum(fock_rows[:, None, :, :] * near_table, axis=(2, 3))
    same = neighbours[:, :, None] == neighbours[:, None, :]
    summed = jnp.sum(jnp.where(same, values[:, None, :], 0.0), axis=2)
    rounded = summed.astype(jnp.bfloat16).astype(jnp.float32)
    slot_ids = jnp.arange(slots, dtype=jnp.int32)
    earlier = same & (slot_ids[None, None, :] < slot_ids[None, :, None])
    repeated = jnp.any(earlier, axis=2)
    return jnp.where(repeated, 0.0, rounded), own_table


def row_of(values):
    flat = values.reshape(1, -1)
    return jnp.pad(flat, ((0, 0), (0, 128 - flat.shape[1])))


def body(
    panels,
    amplitudes,
    drive,
    pno_energy,
    occ_energy,
    frequency,
    pair_lmo,
    neighbours,
    pno_ranks,
    fock_off,
):
    local_pairs, rank_dim, aux_width = panels.shape
    first_pair = lax.axis_index("pair") * local_pairs
    aux = lax.axis_index("aux")
    chip, core = aux // 2, lax.rem(aux, 2)
    rows_index = jnp.arange(rank_dim, dtype=jnp.int32)
    keep_rows = rows_index[None, :] < pno_ranks[:, None]
    masked = jnp.where(keep_rows[:, :, None], panels, jnp.zeros_like(panels))
    masked = masked.reshape(local_pairs, 8, 15, aux_width)
    masked = jnp.pad(masked, ((0, 0), (0, 0), (0, 1), (0, 0)))
    mt = jnp.transpose(masked.reshape(local_pairs, 128, aux_width), (0, 2, 1))
    weights, own_table = slot_weights(pair_lmo, neighbours, fock_off, first_pair)
    piece = lax.dynamic_slice(
        amplitudes, (core, 0, chip * 15, 0), (1, 2, 15, rank_dim)
    )[0]
    piece = jnp.pad(jnp.transpose(piece, (1, 0, 2)), ((0, 1), (0, 0), (0, 8)))
    rows = coupled_rows(mt, piece.reshape(16, 256), row_of(neighbours), row_of(weights))
    rows = rows.reshape(local_pairs, 16, 2, 128)[:, :15, :, :rank_dim]
    rows = jnp.transpose(rows, (0, 2, 1, 3)).reshape(local_pairs, 2, 15 * rank_dim)
    share_width = drive.shape[2]
    coupled_share = lax.dynamic_slice_in_dim(rows, core * share_width, share_width, 2)
    share_start = aux * share_width
    occ_pair = jnp.sum(own_table * occ_energy[None, None, :], axis=(1, 2))
    shift = pno_energy[:, :, None] + pno_energy[:, None, :] - occ_pair[:, None, None]
    shift_flat = lax.dynamic_slice_in_dim(
        shift.reshape(local_pairs, rank_dim * rank_dim), share_start, share_width, 1
    )
    signs = jnp.array([1.0, -1.0], jnp.float32)
    factor = shift_flat[:, None, :] - signs[None, :, None] * frequency[0]
    amp_flat = amplitudes.reshape(local_pairs, 2, rank_dim * rank_dim)
    amp_share = lax.dynamic_slice_in_dim(amp_flat, share_start, share_width, 2).astype(jnp.float32)
    return drive + factor * amp_share + coupled_share


def solution(mesh):
    placed = (
        P("pair", None, "aux"),
        P("pair", None, None, None),
        P("pair", None, "aux"),
        P("pair", None),
        P(),
        P(),
        P(),
        P("pair", None),
        P("pair"),
        P(),
    )
    return jax.shard_map(
        body, mesh=mesh, in_specs=placed, out_specs=P("pair", None, "aux"), check_vma=False
    )
```

```python
import jax
import jax.numpy as jnp
from jax import lax
from jax.experimental import pallas as pl
from jax.experimental.pallas import tpu as pltpu
from jax.sharding import PartitionSpec as P

MESH = pl.DeviceIdType.MESH

PAIR_STEPS = [(1, 0)] + [(dx, dz) for dz in (1, 7, 2, 6, 3, 5, 4) for dx in (0, 1)]
RING = (1, 3, 2)
GROUPS = 4
SPAN = 8 // GROUPS
EARLY = 10


def kernel(
    panel_ref,
    amplitude_ref,
    energy_in,
    fock_in,
    occ_in,
    freq_in,
    lmo_in,
    near_in,
    rank_in,
    out_ref,
    pbuf,
    inamp,
    energy_ref,
    fock_ref,
    occ_ref,
    freq_ref,
    lmo_ref,
    near_ref,
    rank_ref,
    mt_ref,
    amp_ref,
    nbr_ref,
    wgt_ref,
    diag,
    flat,
    mbuf,
    abuf,
    nbuf,
    wbuf,
    nsm,
    wsm,
    proj,
    mtr,
    coll,
    sa,
    sb,
    ra,
    rb,
    ta,
    tb,
    ca,
    cb,
    vbuf,
    ubuf,
    fin,
    l_sem,
    a_sem,
    b_sem,
    y_sem,
    d_sem,
    m_send,
    m_recv,
    f_send,
    f_recv,
    n_sem,
    w_sem,
    r_send,
    r_recv,
    t_send,
    t_recv,
    u_sem,
    x_sem,
):
    pair = lax.axis_index("pair")
    aux = lax.axis_index("aux")
    xlo, z = pair // 8, lax.rem(pair, 8)
    chip, core = aux // 2, lax.rem(aux, 2)
    y, xhi = chip // 2, lax.rem(chip, 2)
    x = xhi * 2 + xlo
    other = 1 - core

    def at(xx, yy, zz, cc):
        return (lax.rem(xx, 2) * 8 + zz, (yy * 2 + xx // 2) * 2 + cc)

    partner = at(x, y, z, other)

    def pair_to(step):
        dx, dz = step
        return lax.rem(xlo + dx, 2) * 8 + lax.rem(z + dz, 8)

    def pair_from(step):
        dx, dz = step
        return lax.rem(xlo + dx, 2) * 8 + lax.rem(z + 8 - dz, 8)

    def x_to(d):
        return at(lax.rem(x + d, 4), y, z, core)

    def y_to(d):
        return at(x, lax.rem(y + d, 4), z, core)

    def z_to(d):
        return at(x, y, lax.rem(z + d, 8), core)

    barrier = pltpu.get_barrier_semaphore()

    def greet(target):
        pl.semaphore_signal(barrier, inc=1, device_id=target, device_id_type=MESH)

    for step in PAIR_STEPS:
        greet((pair_to(step), aux))
    for d in RING:
        greet(y_to(d))
    greet(at(lax.rem(xhi + 1, 2) * 2 + xlo, y, z, core))
    greet(at(lax.rem(xhi + 1, 2) * 2 + 1 - xlo, y, z, core))
    greet(partner)

    def remote(src, dst, send, recv, target):
        return pltpu.make_async_remote_copy(
            src_ref=src,
            dst_ref=dst,
            send_sem=send,
            recv_sem=recv,
            device_id=target,
            device_id_type=MESH,
        )

    def arrived(ref, sems, target):
        remote(ref, ref, sems.at[0], sems.at[1], target).wait_recv()

    def left(ref, sems, target):
        remote(ref, ref, sems.at[0], sems.at[1], target).wait_send()

    loads = [
        pltpu.make_async_copy(src, dst, l_sem.at[i])
        for i, (src, dst) in enumerate(
            [
                (panel_ref, pbuf),
                (amplitude_ref, inamp),
                (energy_in, energy_ref),
                (fock_in, fock_ref),
                (occ_in, occ_ref),
                (freq_in, freq_ref),
                (lmo_in, lmo_ref),
                (near_in, near_ref),
                (rank_in, rank_ref),
            ]
        )
    ]
    for load in loads:
        load.start()
    for load in loads[1:]:
        load.wait()
    lane = lax.broadcasted_iota(jnp.int32, (1, 128), 1)
    near_row = jnp.zeros((1, 128), jnp.int32)
    weight_row = jnp.zeros((1, 128), jnp.float32)
    for c in range(2):
        l0, l1 = lmo_ref[0, 2 * pair + c], lmo_ref[1, 2 * pair + c]
        near = [near_ref[c, k] for k in range(8)]
        value = [fock_ref[l0, lmo_ref[0, n]] + fock_ref[l1, lmo_ref[1, n]] for n in near]
        for k in range(8):
            weight = value[k]
            for j in range(k + 1, 8):
                weight = weight + jnp.where(near[j] == near[k], value[j], 0.0)
            for j in range(k):
                weight = jnp.where(near[j] == near[k], 0.0, weight)
            here = lane == c * 8 + k
            near_row = jnp.where(here, near[k], near_row)
            weight_row = jnp.where(here, weight, weight_row)
    weight_row = weight_row.astype(jnp.bfloat16).astype(jnp.float32)
    nbr_ref[...] = near_row
    wgt_ref[...] = weight_row
    nbuf[pair] = near_row
    wbuf[pair] = weight_row
    slot_row = lax.broadcasted_iota(jnp.int32, (16, 120), 0)
    slot_col = lax.broadcasted_iota(jnp.int32, (16, 120), 1)
    pick = ((slot_row < 15) & (slot_col == chip * 15 + slot_row)).astype(jnp.float32)
    pick16 = pick.astype(jnp.bfloat16)
    amp_ref[...] = jnp.zeros_like(amp_ref)
    for s in range(2):
        rows = jnp.dot(pick16, inamp[core, s], preferred_element_type=jnp.float32)
        amp_ref[:, s * 128 : s * 128 + 120] = rows.astype(jnp.bfloat16)
    abuf[chip, core, pair] = amp_ref[...]
    loads[0].wait()
    place_row = lax.broadcasted_iota(jnp.int32, (128, 120), 0)
    place_col = lax.broadcasted_iota(jnp.int32, (128, 120), 1)
    fill = lax.rem(place_row, 16)
    source = place_row // 16 * 15 + fill
    for c in range(2):
        keep = (fill < 15) & (source == place_col) & (place_col < rank_ref[c])
        place = keep.astype(jnp.float32).astype(jnp.bfloat16)
        for t in range(9):
            cols = pl.ds(t * 256, 256)
            moved = jnp.dot(place, pbuf[c, :, cols], preferred_element_type=jnp.float32)
            mt_ref[c, cols, :] = moved.astype(jnp.bfloat16).T
    pl.semaphore_wait(barrier, 21)

    def m_rows(p):
        return mt_ref.at[:, pl.ds(pl.multiple_of(p * 144, 16), 144), :]

    for dz in (1, 7, 2, 6, 3, 5, 4):
        remote(amp_ref, abuf.at[chip, core, pair], a_sem.at[0], a_sem.at[1], z_to(dz)).start()
    for i, step in enumerate(PAIR_STEPS):
        p = pair_to(step)
        remote(m_rows(p), mbuf.at[pair, core], m_send, m_recv.at[i], (p, aux)).start()
    remote(m_rows(pair), mbuf.at[pair, core], f_send, f_recv.at[15], partner).start()
    for i, step in enumerate(PAIR_STEPS):
        to = (pair_to(step), aux)
        remote(nbr_ref, nbuf.at[pair], n_sem.at[0], n_sem.at[1], to).start()
        remote(wgt_ref, wbuf.at[pair], w_sem.at[0], w_sem.at[1], to).start()
    mbuf[pair, core] = mt_ref[:, pl.ds(pl.multiple_of(pair * 144, 16), 144), :]
    diag[...] = jnp.zeros_like(diag)
    for c in range(2):
        across = energy_ref[pl.ds(c, 1), :]
        down = jnp.sum(pick * across, axis=1, keepdims=True)
        occ = occ_ref[lmo_ref[0, 2 * pair + c]] + occ_ref[lmo_ref[1, 2 * pair + c]]
        shift = down + across - occ
        for s in range(2):
            rows = jnp.dot(pick16, inamp[c, s], preferred_element_type=jnp.float32)
            sign = 1.0 - 2.0 * s
            diag[c, s, :, :120] = (shift - sign * freq_ref[0]) * rows

    def relay_block(i):
        step = PAIR_STEPS[i]
        p = pair_from(step)
        block = mbuf.at[p, core]
        remote(block, block, m_send, m_recv.at[i], (p, aux)).wait_recv()
        remote(block, block, f_send, f_recv.at[i], partner).start()

    def relayed(i):
        p = pair if i == 15 else pair_from(PAIR_STEPS[i])
        block = mbuf.at[p, other]
        remote(block, block, f_send, f_recv.at[i], partner).wait_recv()
        for h in range(2):
            mtr[p, h] = mbuf[p, h, core].T
        return p

    def project(p):
        for c in range(2):
            matrix = abuf[:, c, p].reshape(128, 256)
            for h in range(2):
                proj[2 * p + c, h] = jnp.dot(
                    mbuf[p, h, c], matrix, preferred_element_type=jnp.float32
                ).astype(jnp.bfloat16)

    def column(xx):
        return abuf.at[y * 2 + xx // 2, core, pl.ds(lax.rem(xx, 2) * 8, 8)]

    def rows_of(yy, cc):
        return abuf.at[pl.ds(yy * 2, 2), cc]

    relayed(15)
    relay_block(0)
    relay_block(1)
    arrived(abuf.at[0, 0, pl.ds(0, 7)], a_sem, partner)
    for d in RING:
        remote(column(x), column(x), b_sem.at[0], b_sem.at[1], x_to(d)).start()
    for d in RING:
        remote(column(x), column(x), y_sem.at[0], y_sem.at[1], y_to(d)).start()
    relay_block(2)
    relayed(0)
    relayed(1)
    arrived(abuf.at[pl.ds(0, 3), 0, pl.ds(0, 8)], b_sem, partner)
    for e in RING:
        for d in RING:
            xx = lax.rem(x + e, 4)
            remote(column(xx), column(xx), y_sem.at[0], y_sem.at[1], y_to(d)).start()
    remote(rows_of(y, core), rows_of(y, core), d_sem.at[0], d_sem.at[1], partner).start()
    for i in range(3, EARLY):
        relay_block(i)
        relayed(i - 1)
    arrived(abuf.at[pl.ds(0, 6), 0], y_sem, partner)
    for d in RING:
        yy = lax.rem(y + d, 4)
        remote(rows_of(yy, core), rows_of(yy, core), d_sem.at[0], d_sem.at[1], partner).start()
    relayed(EARLY - 1)
    relay_block(EARLY)
    arrived(nbuf.at[pl.ds(0, 15)], n_sem, partner)
    arrived(wbuf.at[pl.ds(0, 15)], w_sem, partner)
    to_nsm = pltpu.make_async_copy(nbuf, nsm, l_sem.at[0])
    to_wsm = pltpu.make_async_copy(wbuf, wsm, l_sem.at[1])
    to_nsm.start()
    to_wsm.start()
    to_nsm.wait()
    to_wsm.wait()
    arrived(abuf.at[:, 0], d_sem, partner)
    project(pair)
    for i in range(EARLY):
        project(pair_from(PAIR_STEPS[i]))
    for i in range(EARLY, 15):
        if i + 1 < 15:
            relay_block(i + 1)
        project(relayed(i))

    def close(lo, zz):
        p = lo * 8 + zz
        for h in range(2):
            total = jnp.zeros((144, 256), jnp.float32)
            for k in range(8):
                n = nsm[p, 0, core * 8 + k]
                w = wsm[p, 0, core * 8 + k]
                total = total + w * proj[n, h].astype(jnp.float32)
            coll[lo, h] = total.astype(jnp.bfloat16)
        closed = jnp.dot(mtr[p, 0], coll[lo, 0], preferred_element_type=jnp.float32)
        closed = closed + jnp.dot(mtr[p, 1], coll[lo, 1], preferred_element_type=jnp.float32)
        closed = closed.astype(jnp.bfloat16).reshape(4, 2, 16, 256)
        sa[:, :, lo, zz] = closed[:, :, :, :128]
        for hi in range(2):
            sb[hi, lo, :, zz] = closed[:, hi, :, 128:]

    def close_both(zz, carry):
        close(0, zz)
        close(1, zz)
        return carry

    def span(q):
        return pl.ds(q * SPAN, SPAN)

    for q in range(GROUPS):
        lax.fori_loop(q * SPAN, (q + 1) * SPAN, close_both, 0)
        for i, d in enumerate(RING):
            yy, xx = lax.rem(y + d, 4), lax.rem(x + d, 4)
            remote(
                sa.at[yy, :, :, span(q)],
                ra.at[i, :, :, span(q)],
                r_send.at[0],
                r_recv.at[0, q],
                y_to(d),
            ).start()
            remote(
                sb.at[xx // 2, lax.rem(xx, 2), :, span(q)],
                rb.at[i, :, span(q)],
                r_send.at[1],
                r_recv.at[1, q],
                x_to(d),
            ).start()

    def first_sum(q):
        part = ra.at[:, :, :, span(q)]
        remote(part, part, r_send.at[0], r_recv.at[0, q], partner).wait_recv()
        total = sa[y, :, :, span(q)].astype(jnp.float32)
        for i in range(3):
            total = total + ra[i, :, :, span(q)].astype(jnp.float32)
        ta[:, :, span(q)] = total.astype(jnp.bfloat16)
        for i, d in enumerate(RING):
            xx = lax.rem(x + d, 4)
            remote(
                ta.at[xx // 2, lax.rem(xx, 2), span(q)],
                ca.at[i, span(q)],
                t_send.at[0],
                t_recv.at[0, q],
                x_to(d),
            ).start()
        part = rb.at[:, :, span(q)]
        remote(part, part, r_send.at[1], r_recv.at[1, q], partner).wait_recv()
        total = sb[xhi, xlo, :, span(q)].astype(jnp.float32)
        for i in range(3):
            total = total + rb[i, :, span(q)].astype(jnp.float32)
        tb[:, span(q)] = total.astype(jnp.bfloat16)
        for i, d in enumerate(RING):
            yy = lax.rem(y + d, 4)
            remote(
                tb.at[yy, span(q)],
                cb.at[i, span(q)],
                t_send.at[1],
                t_recv.at[1, q],
                y_to(d),
            ).start()

    def second_sum(q):
        part = ca.at[:, span(q)]
        remote(part, part, t_send.at[0], t_recv.at[0, q], partner).wait_recv()
        total = ta[xhi, xlo, span(q)].astype(jnp.float32)
        for i in range(3):
            total = total + ca[i, span(q)].astype(jnp.float32)
        vbuf[span(q), 0] = total.astype(jnp.bfloat16)
        part = cb.at[:, span(q)]
        remote(part, part, t_send.at[1], t_recv.at[1, q], partner).wait_recv()
        total = tb[y, span(q)].astype(jnp.float32)
        for i in range(3):
            total = total + cb[i, span(q)].astype(jnp.float32)
        vbuf[span(q), 1] = total.astype(jnp.bfloat16)
        for j in range(SPAN):
            zz = q * SPAN + j

            @pl.when(zz != z)
            def _():
                slot = lax.rem(zz - z + 8, 8) - 1
                remote(
                    vbuf.at[zz], ubuf.at[slot], u_sem.at[0], u_sem.at[1], at(x, y, zz, core)
                ).start()

    first_sum(0)
    for q in range(1, GROUPS):
        first_sum(q)
        second_sum(q - 1)
    second_sum(GROUPS - 1)
    arrived(ubuf, u_sem, partner)
    total = vbuf[z].astype(jnp.float32)
    for slot in range(7):
        total = total + ubuf[slot].astype(jnp.float32)
    fin[core] = total
    swap = remote(fin.at[core], fin.at[core], x_sem.at[0], x_sem.at[1], partner)
    swap.start()
    remote(fin.at[other], fin.at[other], x_sem.at[0], x_sem.at[1], partner).wait_recv()
    for c in range(2):
        for s in range(2):
            rows = fin[c, s] + diag[c, s]
            line = slice(2 * c + s, 2 * c + s + 1)
            for j in range(8):
                row = jnp.where(core == 0, rows[j : j + 1, :120], rows[j + 7 : j + 8, :120])
                flat[line, j * 120 : j * 120 + 120] = row
            whole = flat[line, :]
            out_ref[c, s : s + 1, :] = jnp.where(core == 0, whole[:, :900], whole[:, 60:960])
    left(abuf.at[0, 0, pl.ds(0, 7)], a_sem, partner)
    left(abuf.at[pl.ds(0, 3), 0, pl.ds(0, 8)], b_sem, partner)
    left(abuf.at[pl.ds(0, 6), 0], y_sem, partner)
    left(abuf.at[:, 0], d_sem, partner)
    left(nbuf.at[pl.ds(0, 15)], n_sem, partner)
    left(wbuf.at[pl.ds(0, 15)], w_sem, partner)
    left(ubuf, u_sem, partner)
    blocks = mbuf.at[pl.ds(0, 15), 0]
    remote(blocks, blocks, m_send, m_recv.at[0], partner).wait_send()
    blocks = mbuf.at[:, 0]
    remote(blocks, blocks, f_send, f_recv.at[0], partner).wait_send()
    for half, (one, two) in enumerate([(ra, ca), (rb, cb)]):
        remote(one, one, r_send.at[half], r_recv.at[half, 0], partner).wait_send()
        remote(two, two, t_send.at[half], t_recv.at[half, 0], partner).wait_send()
    swap.wait_send()


def coupled_rows(*operands):
    bf16, f32, i32 = jnp.bfloat16, jnp.float32, jnp.int32
    dma = pltpu.SemaphoreType.DMA
    vmem, hbm = pl.BlockSpec(memory_space=pltpu.VMEM), pl.BlockSpec(memory_space=pl.ANY)
    return pl.pallas_call(
        kernel,
        out_shape=jax.ShapeDtypeStruct((2, 2, 900), f32),
        in_specs=[hbm] * 9,
        out_specs=vmem,
        scratch_shapes=[
            pltpu.VMEM((2, 120, 2304), bf16),
            pltpu.VMEM((2, 2, 120, 120), bf16),
            pltpu.VMEM((2, 120), f32),
            pltpu.SMEM((64, 64), f32),
            pltpu.SMEM((64,), f32),
            pltpu.SMEM((1,), f32),
            pltpu.SMEM((2, 32), i32),
            pltpu.SMEM((2, 8), i32),
            pltpu.SMEM((2,), i32),
            pltpu.VMEM((2, 2304, 128), bf16),
            pltpu.VMEM((16, 256), bf16),
            pltpu.VMEM((1, 128), i32),
            pltpu.VMEM((1, 128), f32),
            pltpu.VMEM((2, 2, 16, 128), f32),
            pltpu.VMEM((4, 1024), f32),
            pltpu.VMEM((16, 2, 2, 144, 128), bf16),
            pltpu.VMEM((8, 2, 16, 16, 256), bf16),
            pltpu.VMEM((16, 1, 128), i32),
            pltpu.VMEM((16, 1, 128), f32),
            pltpu.SMEM((16, 1, 128), i32),
            pltpu.SMEM((16, 1, 128), f32),
            pltpu.VMEM((32, 2, 144, 256), bf16),
            pltpu.VMEM((16, 2, 128, 144), bf16),
            pltpu.VMEM((2, 2, 144, 256), bf16),
            pltpu.VMEM((4, 2, 2, 8, 16, 128), bf16),
            pltpu.VMEM((2, 2, 4, 8, 16, 128), bf16),
            pltpu.VMEM((3, 2, 2, 8, 16, 128), bf16),
            pltpu.VMEM((3, 4, 8, 16, 128), bf16),
            pltpu.VMEM((2, 2, 8, 16, 128), bf16),
            pltpu.VMEM((4, 8, 16, 128), bf16),
            pltpu.VMEM((3, 8, 16, 128), bf16),
            pltpu.VMEM((3, 8, 16, 128), bf16),
            pltpu.VMEM((8, 2, 16, 128), bf16),
            pltpu.VMEM((7, 2, 16, 128), bf16),
            pltpu.VMEM((2, 2, 16, 128), f32),
            dma((9,)),
            dma((2,)),
            dma((2,)),
            dma((2,)),
            dma((2,)),
            dma,
            dma((15,)),
            dma,
            dma((16,)),
            dma((2,)),
            dma((2,)),
            dma((2,)),
            dma((2, GROUPS)),
            dma((2,)),
            dma((2, GROUPS)),
            dma((2,)),
            dma((2,)),
        ],
        compiler_params=pltpu.CompilerParams(
            collective_id=0, has_side_effects=True, vmem_limit_bytes=56 << 20
        ),
        name="coupled_rows",
    )(*operands)


def body(
    panels,
    amplitudes,
    drive,
    pno_energy,
    occ_energy,
    frequency,
    pair_lmo,
    neighbours,
    pno_ranks,
    fock_off,
):
    return drive + coupled_rows(
        panels,
        amplitudes,
        pno_energy,
        fock_off,
        occ_energy,
        frequency,
        pair_lmo.T,
        neighbours,
        pno_ranks,
    )


def solution(mesh):
    placed = (
        P("pair", None, "aux"),
        P("pair", None, None, None),
        P("pair", None, "aux"),
        P("pair", None),
        P(),
        P(),
        P(),
        P("pair", None),
        P("pair"),
        P(),
    )
    return jax.shard_map(
        body, mesh=mesh, in_specs=placed, out_specs=P("pair", None, "aux"), check_vma=False
    )
```

```python
import jax
import jax.numpy as jnp
from jax import lax
from jax.experimental import pallas as pl
from jax.experimental.pallas import tpu as pltpu
from jax.sharding import PartitionSpec as P

MESH = pl.DeviceIdType.MESH

PAIR_STEPS = [(1, 0)] + [(dx, dz) for dz in (1, 7, 2, 6, 3, 5, 4) for dx in (0, 1)]
RING = (1, 3, 2)
GROUPS = 4
SPAN = 8 // GROUPS
EARLY = 10


def kernel(
    panel_ref,
    amplitude_ref,
    energy_in,
    fock_in,
    occ_in,
    freq_in,
    lmo_in,
    near_in,
    rank_in,
    out_ref,
    pbuf,
    inamp,
    energy_ref,
    fock_ref,
    occ_ref,
    freq_ref,
    lmo_ref,
    near_ref,
    rank_ref,
    mt_ref,
    amp_ref,
    nbr_ref,
    wgt_ref,
    diag,
    flat,
    mbuf,
    abuf,
    nbuf,
    wbuf,
    nsm,
    wsm,
    proj,
    mtr,
    coll,
    sa,
    sb,
    ra,
    rb,
    ta,
    tb,
    ca,
    cb,
    vbuf,
    ubuf,
    l_sem,
    a_sem,
    b_sem,
    y_sem,
    d_sem,
    m_send,
    m_recv,
    f_send,
    f_recv,
    n_sem,
    w_sem,
    r_send,
    r_recv,
    t_send,
    t_recv,
    u_sem,
):
    pair = lax.axis_index("pair")
    aux = lax.axis_index("aux")
    xlo, z = pair // 8, lax.rem(pair, 8)
    chip, core = aux // 2, lax.rem(aux, 2)
    y, xhi = chip // 2, lax.rem(chip, 2)
    x = xhi * 2 + xlo
    other = 1 - core

    def at(xx, yy, zz, cc):
        return (lax.rem(xx, 2) * 8 + zz, (yy * 2 + xx // 2) * 2 + cc)

    partner = at(x, y, z, other)

    def pair_to(step):
        dx, dz = step
        return lax.rem(xlo + dx, 2) * 8 + lax.rem(z + dz, 8)

    def pair_from(step):
        dx, dz = step
        return lax.rem(xlo + dx, 2) * 8 + lax.rem(z + 8 - dz, 8)

    def x_to(d):
        return at(lax.rem(x + d, 4), y, z, core)

    def y_to(d):
        return at(x, lax.rem(y + d, 4), z, core)

    def z_to(d):
        return at(x, y, lax.rem(z + d, 8), core)

    barrier = pltpu.get_barrier_semaphore()

    def greet(target):
        pl.semaphore_signal(barrier, inc=1, device_id=target, device_id_type=MESH)

    for step in PAIR_STEPS:
        greet((pair_to(step), aux))
    for d in RING:
        greet(y_to(d))
    greet(at(lax.rem(xhi + 1, 2) * 2 + xlo, y, z, core))
    greet(at(lax.rem(xhi + 1, 2) * 2 + 1 - xlo, y, z, core))
    greet(partner)
    for dz in range(1, 8):
        greet(at(x, y, lax.rem(z + dz, 8), other))

    def remote(src, dst, send, recv, target):
        return pltpu.make_async_remote_copy(
            src_ref=src,
            dst_ref=dst,
            send_sem=send,
            recv_sem=recv,
            device_id=target,
            device_id_type=MESH,
        )

    def arrived(ref, sems, target):
        remote(ref, ref, sems.at[0], sems.at[1], target).wait_recv()

    def left(ref, sems, target):
        remote(ref, ref, sems.at[0], sems.at[1], target).wait_send()

    loads = [
        pltpu.make_async_copy(src, dst, l_sem.at[i])
        for i, (src, dst) in enumerate(
            [
                (panel_ref, pbuf),
                (amplitude_ref, inamp),
                (energy_in, energy_ref),
                (fock_in, fock_ref),
                (occ_in, occ_ref),
                (freq_in, freq_ref),
                (lmo_in, lmo_ref),
                (near_in, near_ref),
                (rank_in, rank_ref),
            ]
        )
    ]
    for load in loads:
        load.start()
    for load in loads[1:]:
        load.wait()
    lane = lax.broadcasted_iota(jnp.int32, (1, 128), 1)
    near_row = jnp.zeros((1, 128), jnp.int32)
    weight_row = jnp.zeros((1, 128), jnp.float32)
    for c in range(2):
        l0, l1 = lmo_ref[0, 2 * pair + c], lmo_ref[1, 2 * pair + c]
        near = [near_ref[c, k] for k in range(8)]
        value = [fock_ref[l0, lmo_ref[0, n]] + fock_ref[l1, lmo_ref[1, n]] for n in near]
        for k in range(8):
            weight = value[k]
            for j in range(k + 1, 8):
                weight = weight + jnp.where(near[j] == near[k], value[j], 0.0)
            for j in range(k):
                weight = jnp.where(near[j] == near[k], 0.0, weight)
            here = lane == c * 8 + k
            near_row = jnp.where(here, near[k], near_row)
            weight_row = jnp.where(here, weight, weight_row)
    weight_row = weight_row.astype(jnp.bfloat16).astype(jnp.float32)
    nbr_ref[...] = near_row
    wgt_ref[...] = weight_row
    nbuf[pair] = near_row
    wbuf[pair] = weight_row
    slot_row = lax.broadcasted_iota(jnp.int32, (16, 120), 0)
    slot_col = lax.broadcasted_iota(jnp.int32, (16, 120), 1)
    pick = ((slot_row < 15) & (slot_col == chip * 15 + slot_row)).astype(jnp.float32)
    pick16 = pick.astype(jnp.bfloat16)
    amp_ref[...] = jnp.zeros_like(amp_ref)
    for s in range(2):
        rows = jnp.dot(pick16, inamp[core, s], preferred_element_type=jnp.float32)
        amp_ref[:, s * 128 : s * 128 + 120] = rows.astype(jnp.bfloat16)
    abuf[chip, core, pair] = amp_ref[...]
    loads[0].wait()
    place_row = lax.broadcasted_iota(jnp.int32, (128, 120), 0)
    place_col = lax.broadcasted_iota(jnp.int32, (128, 120), 1)
    fill = lax.rem(place_row, 16)
    source = place_row // 16 * 15 + fill
    for c in range(2):
        keep = (fill < 15) & (source == place_col) & (place_col < rank_ref[c])
        place = keep.astype(jnp.float32).astype(jnp.bfloat16)
        for t in range(9):
            cols = pl.ds(t * 256, 256)
            moved = jnp.dot(place, pbuf[c, :, cols], preferred_element_type=jnp.float32)
            mt_ref[c, cols, :] = moved.astype(jnp.bfloat16).T
    pl.semaphore_wait(barrier, 28)

    def m_rows(p):
        return mt_ref.at[:, pl.ds(pl.multiple_of(p * 144, 16), 144), :]

    for dz in (1, 7, 2, 6, 3, 5, 4):
        remote(amp_ref, abuf.at[chip, core, pair], a_sem.at[0], a_sem.at[1], z_to(dz)).start()
    for i, step in enumerate(PAIR_STEPS):
        to = (pair_to(step), aux)
        remote(nbr_ref, nbuf.at[pair], n_sem.at[0], n_sem.at[1], to).start()
        remote(wgt_ref, wbuf.at[pair], w_sem.at[0], w_sem.at[1], to).start()
    for i, step in enumerate(PAIR_STEPS):
        p = pair_to(step)
        remote(m_rows(p), mbuf.at[pair, core], m_send, m_recv.at[i], (p, aux)).start()
    remote(m_rows(pair), mbuf.at[pair, core], f_send, f_recv.at[15], partner).start()
    mbuf[pair, core] = mt_ref[:, pl.ds(pl.multiple_of(pair * 144, 16), 144), :]
    diag[...] = jnp.zeros_like(diag)
    own_row = lax.broadcasted_iota(jnp.int32, (8, 120), 0) + chip * 15 + core * 7
    own = (lax.broadcasted_iota(jnp.int32, (8, 120), 1) == own_row).astype(jnp.float32)
    for c in range(2):
        across = energy_ref[pl.ds(c, 1), :]
        down = jnp.sum(own * across, axis=1, keepdims=True)
        occ = occ_ref[lmo_ref[0, 2 * pair + c]] + occ_ref[lmo_ref[1, 2 * pair + c]]
        shift = down + across - occ
        for s in range(2):
            rows = jnp.dot(
                own.astype(jnp.bfloat16), inamp[c, s], preferred_element_type=jnp.float32
            )
            sign = 1.0 - 2.0 * s
            diag[c, s, :, :120] = (shift - sign * freq_ref[0]) * rows

    def relay_block(i):
        step = PAIR_STEPS[i]
        p = pair_from(step)
        block = mbuf.at[p, core]
        remote(block, block, m_send, m_recv.at[i], (p, aux)).wait_recv()
        remote(block, block, f_send, f_recv.at[i], partner).start()

    def relayed(i):
        p = pair if i == 15 else pair_from(PAIR_STEPS[i])
        block = mbuf.at[p, other]
        remote(block, block, f_send, f_recv.at[i], partner).wait_recv()
        for h in range(2):
            mtr[p, h] = mbuf[p, h, core].T
        return p

    def project(p):
        for c in range(2):
            matrix = abuf[:, c, p].reshape(128, 256)
            for h in range(2):
                block = jnp.dot(mbuf[p, h, c], matrix, preferred_element_type=jnp.float32)
                proj[2 * p + c, h] = block.astype(jnp.bfloat16).astype(jnp.float32)

    def column(xx):
        return abuf.at[y * 2 + xx // 2, core, pl.ds(lax.rem(xx, 2) * 8, 8)]

    def rows_of(yy, cc):
        return abuf.at[pl.ds(yy * 2, 2), cc]

    relayed(15)
    relay_block(0)
    relay_block(1)
    arrived(abuf.at[0, 0, pl.ds(0, 7)], a_sem, partner)
    for d in RING:
        remote(column(x), column(x), b_sem.at[0], b_sem.at[1], x_to(d)).start()
    for d in RING:
        remote(column(x), column(x), y_sem.at[0], y_sem.at[1], y_to(d)).start()
    relay_block(2)
    relayed(0)
    relayed(1)
    arrived(abuf.at[pl.ds(0, 3), 0, pl.ds(0, 8)], b_sem, partner)
    for e in RING:
        for d in RING:
            xx = lax.rem(x + e, 4)
            remote(column(xx), column(xx), y_sem.at[0], y_sem.at[1], y_to(d)).start()
    remote(rows_of(y, core), rows_of(y, core), d_sem.at[0], d_sem.at[1], partner).start()
    for i in range(3, EARLY):
        relay_block(i)
        relayed(i - 1)
    arrived(abuf.at[pl.ds(0, 6), 0], y_sem, partner)
    for d in RING:
        yy = lax.rem(y + d, 4)
        remote(rows_of(yy, core), rows_of(yy, core), d_sem.at[0], d_sem.at[1], partner).start()
    relayed(EARLY - 1)
    relay_block(EARLY)
    arrived(nbuf.at[pl.ds(0, 15)], n_sem, partner)
    arrived(wbuf.at[pl.ds(0, 15)], w_sem, partner)
    to_nsm = pltpu.make_async_copy(nbuf, nsm, l_sem.at[0])
    to_wsm = pltpu.make_async_copy(wbuf, wsm, l_sem.at[1])
    to_nsm.start()
    to_wsm.start()
    to_nsm.wait()
    to_wsm.wait()
    arrived(abuf.at[:, 0], d_sem, partner)
    project(pair)
    for i in range(EARLY):
        project(pair_from(PAIR_STEPS[i]))
    for i in range(EARLY, 15):
        if i + 1 < 15:
            relay_block(i + 1)
        project(relayed(i))

    def close(lo, zz):
        p = lo * 8 + zz
        for h in range(2):
            total = jnp.zeros((144, 256), jnp.float32)
            for k in range(8):
                n = nsm[p, 0, core * 8 + k]
                w = wsm[p, 0, core * 8 + k]
                total = total + w * proj[n, h]
            coll[lo, h] = total.astype(jnp.bfloat16)
        closed = jnp.dot(mtr[p, 0], coll[lo, 0], preferred_element_type=jnp.float32)
        closed = closed + jnp.dot(mtr[p, 1], coll[lo, 1], preferred_element_type=jnp.float32)
        closed = closed.astype(jnp.bfloat16).reshape(4, 2, 16, 256)
        sa[:, :, lo, zz] = closed[:, :, :, :128]
        for hi in range(2):
            sb[hi, lo, :, zz] = closed[:, hi, :, 128:]

    def close_both(zz, carry):
        close(0, zz)
        close(1, zz)
        return carry

    def span(q):
        return pl.ds(q * SPAN, SPAN)

    for q in range(GROUPS):
        lax.fori_loop(q * SPAN, (q + 1) * SPAN, close_both, 0)
        for i, d in enumerate(RING):
            yy, xx = lax.rem(y + d, 4), lax.rem(x + d, 4)
            remote(
                sa.at[yy, :, :, span(q)],
                ra.at[i, :, :, span(q)],
                r_send.at[0],
                r_recv.at[0, q],
                y_to(d),
            ).start()
            remote(
                sb.at[xx // 2, lax.rem(xx, 2), :, span(q)],
                rb.at[i, :, span(q)],
                r_send.at[1],
                r_recv.at[1, q],
                x_to(d),
            ).start()

    def first_sum(q):
        part = ra.at[:, :, :, span(q)]
        remote(part, part, r_send.at[0], r_recv.at[0, q], partner).wait_recv()
        total = sa[y, :, :, span(q)].astype(jnp.float32)
        for i in range(3):
            total = total + ra[i, :, :, span(q)].astype(jnp.float32)
        ta[:, :, span(q)] = total.astype(jnp.bfloat16)
        for i, d in enumerate(RING):
            xx = lax.rem(x + d, 4)
            remote(
                ta.at[xx // 2, lax.rem(xx, 2), span(q)],
                ca.at[i, span(q)],
                t_send.at[0],
                t_recv.at[0, q],
                x_to(d),
            ).start()
        part = rb.at[:, :, span(q)]
        remote(part, part, r_send.at[1], r_recv.at[1, q], partner).wait_recv()
        total = sb[xhi, xlo, :, span(q)].astype(jnp.float32)
        for i in range(3):
            total = total + rb[i, :, span(q)].astype(jnp.float32)
        tb[:, span(q)] = total.astype(jnp.bfloat16)
        for i, d in enumerate(RING):
            yy = lax.rem(y + d, 4)
            remote(
                tb.at[yy, span(q)],
                cb.at[i, span(q)],
                t_send.at[1],
                t_recv.at[1, q],
                y_to(d),
            ).start()

    def second_sum(q):
        part = ca.at[:, span(q)]
        remote(part, part, t_send.at[0], t_recv.at[0, q], partner).wait_recv()
        total = ta[xhi, xlo, span(q)].astype(jnp.float32)
        for i in range(3):
            total = total + ca[i, span(q)].astype(jnp.float32)
        vbuf[span(q), 0, 0] = total[:, :8].astype(jnp.bfloat16)
        vbuf[span(q), 1, 0] = total[:, 7:15].astype(jnp.bfloat16)
        part = cb.at[:, span(q)]
        remote(part, part, t_send.at[1], t_recv.at[1, q], partner).wait_recv()
        total = tb[y, span(q)].astype(jnp.float32)
        for i in range(3):
            total = total + cb[i, span(q)].astype(jnp.float32)
        vbuf[span(q), 0, 1] = total[:, :8].astype(jnp.bfloat16)
        vbuf[span(q), 1, 1] = total[:, 7:15].astype(jnp.bfloat16)
        for j in range(SPAN):
            zz = q * SPAN + j
            slot = lax.rem(zz - z + 8, 8)
            remote(
                vbuf.at[zz, other],
                ubuf.at[slot * 2 + core],
                u_sem.at[0],
                u_sem.at[1],
                at(x, y, zz, other),
            ).start()

            @pl.when(zz != z)
            def _():
                remote(
                    vbuf.at[zz, core],
                    ubuf.at[slot * 2 + core],
                    u_sem.at[0],
                    u_sem.at[1],
                    at(x, y, zz, core),
                ).start()

    first_sum(0)
    for q in range(1, GROUPS):
        first_sum(q)
        second_sum(q - 1)
    second_sum(GROUPS - 1)
    ubuf[core] = vbuf[z, core]
    arrived(ubuf.at[pl.ds(0, 15)], u_sem, partner)
    for c in range(2):
        total = diag[c]
        for slot in range(8):
            total = total + ubuf[slot * 2 + c].astype(jnp.float32)
        for s in range(2):
            line = slice(2 * c + s, 2 * c + s + 1)
            for j in range(8):
                flat[line, j * 120 : j * 120 + 120] = total[s, j : j + 1, :120]
            whole = flat[line, :]
            out_ref[c, s : s + 1, :] = jnp.where(core == 0, whole[:, :900], whole[:, 60:960])
    left(abuf.at[0, 0, pl.ds(0, 7)], a_sem, partner)
    left(abuf.at[pl.ds(0, 3), 0, pl.ds(0, 8)], b_sem, partner)
    left(abuf.at[pl.ds(0, 6), 0], y_sem, partner)
    left(abuf.at[:, 0], d_sem, partner)
    left(nbuf.at[pl.ds(0, 15)], n_sem, partner)
    left(wbuf.at[pl.ds(0, 15)], w_sem, partner)
    left(ubuf.at[pl.ds(0, 15)], u_sem, partner)
    blocks = mbuf.at[pl.ds(0, 15), 0]
    remote(blocks, blocks, m_send, m_recv.at[0], partner).wait_send()
    blocks = mbuf.at[:, 0]
    remote(blocks, blocks, f_send, f_recv.at[0], partner).wait_send()
    for half, (one, two) in enumerate([(ra, ca), (rb, cb)]):
        remote(one, one, r_send.at[half], r_recv.at[half, 0], partner).wait_send()
        remote(two, two, t_send.at[half], t_recv.at[half, 0], partner).wait_send()


def coupled_rows(*operands):
    bf16, f32, i32 = jnp.bfloat16, jnp.float32, jnp.int32
    dma = pltpu.SemaphoreType.DMA
    vmem, hbm = pl.BlockSpec(memory_space=pltpu.VMEM), pl.BlockSpec(memory_space=pltpu.HBM)
    return pl.pallas_call(
        kernel,
        out_shape=jax.ShapeDtypeStruct((2, 2, 900), f32),
        in_specs=[hbm] * 9,
        out_specs=vmem,
        scratch_shapes=[
            pltpu.VMEM((2, 120, 2304), bf16),
            pltpu.VMEM((2, 2, 120, 120), bf16),
            pltpu.VMEM((2, 120), f32),
            pltpu.SMEM((64, 64), f32),
            pltpu.SMEM((64,), f32),
            pltpu.SMEM((1,), f32),
            pltpu.SMEM((2, 32), i32),
            pltpu.SMEM((2, 8), i32),
            pltpu.SMEM((2,), i32),
            pltpu.VMEM((2, 2304, 128), bf16),
            pltpu.VMEM((16, 256), bf16),
            pltpu.VMEM((1, 128), i32),
            pltpu.VMEM((1, 128), f32),
            pltpu.VMEM((2, 2, 8, 128), f32),
            pltpu.VMEM((4, 1024), f32),
            pltpu.VMEM((16, 2, 2, 144, 128), bf16),
            pltpu.VMEM((8, 2, 16, 16, 256), bf16),
            pltpu.VMEM((16, 1, 128), i32),
            pltpu.VMEM((16, 1, 128), f32),
            pltpu.SMEM((16, 1, 128), i32),
            pltpu.SMEM((16, 1, 128), f32),
            pltpu.VMEM((32, 2, 144, 256), f32),
            pltpu.VMEM((16, 2, 128, 144), bf16),
            pltpu.VMEM((2, 2, 144, 256), bf16),
            pltpu.VMEM((4, 2, 2, 8, 16, 128), bf16),
            pltpu.VMEM((2, 2, 4, 8, 16, 128), bf16),
            pltpu.VMEM((3, 2, 2, 8, 16, 128), bf16),
            pltpu.VMEM((3, 4, 8, 16, 128), bf16),
            pltpu.VMEM((2, 2, 8, 16, 128), bf16),
            pltpu.VMEM((4, 8, 16, 128), bf16),
            pltpu.VMEM((3, 8, 16, 128), bf16),
            pltpu.VMEM((3, 8, 16, 128), bf16),
            pltpu.VMEM((8, 2, 2, 8, 128), bf16),
            pltpu.VMEM((16, 2, 8, 128), bf16),
            dma((9,)),
            dma((2,)),
            dma((2,)),
            dma((2,)),
            dma((2,)),
            dma,
            dma((15,)),
            dma,
            dma((16,)),
            dma((2,)),
            dma((2,)),
            dma((2,)),
            dma((2, GROUPS)),
            dma((2,)),
            dma((2, GROUPS)),
            dma((2,)),
        ],
        compiler_params=pltpu.CompilerParams(
            collective_id=0, has_side_effects=True, vmem_limit_bytes=28 << 20
        ),
        name="coupled_rows",
    )(*[o if o.size == 1 else pltpu.with_memory_space_constraint(o, pltpu.HBM) for o in operands])


def body(
    panels,
    amplitudes,
    drive,
    pno_energy,
    occ_energy,
    frequency,
    pair_lmo,
    neighbours,
    pno_ranks,
    fock_off,
):
    return drive + coupled_rows(
        panels,
        amplitudes,
        pno_energy,
        fock_off,
        occ_energy,
        frequency,
        pair_lmo.T,
        neighbours,
        pno_ranks,
    )


def solution(mesh):
    placed = (
        P("pair", None, "aux"),
        P("pair", None, None, None),
        P("pair", None, "aux"),
        P("pair", None),
        P(),
        P(),
        P(),
        P("pair", None),
        P("pair"),
        P(),
    )
    return jax.shard_map(
        body, mesh=mesh, in_specs=placed, out_specs=P("pair", None, "aux"), check_vma=False
    )
```

```python
import jax
import jax.numpy as jnp
from jax import lax
from jax.experimental import pallas as pl
from jax.experimental.pallas import tpu as pltpu
from jax.sharding import PartitionSpec as P

MESH = pl.DeviceIdType.MESH

PAIR_STEPS = [(0, dz) for dz in (1, 7, 2, 6, 3, 5, 4)]
PAIR_STEPS += [(1, dz) for dz in (0, 1, 7, 2, 6, 3, 5, 4)]
NEAR = 7
RING = (1, 3, 2)
GROUPS = 4
SPAN = 8 // GROUPS
EARLY = 10
LAG = 2
Z_ORDER = (0, 1, 7, 2, 6, 3, 5, 4)


def kernel(
    panel_ref,
    amplitude_ref,
    energy_in,
    fock_in,
    occ_in,
    freq_in,
    lmo_in,
    near_in,
    rank_in,
    out_ref,
    pbuf,
    inamp,
    energy_ref,
    fock_ref,
    occ_ref,
    freq_ref,
    lmo_ref,
    near_ref,
    rank_ref,
    mt_ref,
    amp_ref,
    nbr_ref,
    wgt_ref,
    diag,
    flat,
    mw,
    mbuf,
    nb,
    abuf,
    nbuf,
    wbuf,
    nsm,
    wsm,
    proj,
    mtr,
    coll,
    sa,
    sb,
    ra,
    rb,
    ta,
    tb,
    ca,
    cb,
    vbuf,
    ubuf,
    l_sem,
    a_sem,
    b_sem,
    y_sem,
    d_sem,
    m_send,
    m_recv,
    f_send,
    f_recv,
    n_sem,
    w_sem,
    r_send,
    r_recv,
    t_send,
    t_recv,
    u_sem,
):
    pair = lax.axis_index("pair")
    aux = lax.axis_index("aux")
    xlo, z = pair // 8, lax.rem(pair, 8)
    chip, core = aux // 2, lax.rem(aux, 2)
    y, xhi = chip // 2, lax.rem(chip, 2)
    x = xhi * 2 + xlo
    other = 1 - core

    def at(xx, yy, zz, cc):
        return (lax.rem(xx, 2) * 8 + zz, (yy * 2 + xx // 2) * 2 + cc)

    partner = at(x, y, z, other)

    def pair_to(step):
        dx, dz = step
        return lax.rem(xlo + dx, 2) * 8 + lax.rem(z + dz, 8)

    def pair_from(step):
        dx, dz = step
        return lax.rem(xlo + dx, 2) * 8 + lax.rem(z + 8 - dz, 8)

    def x_to(d):
        return at(lax.rem(x + d, 4), y, z, core)

    def y_to(d):
        return at(x, lax.rem(y + d, 4), z, core)

    def z_to(d):
        return at(x, y, lax.rem(z + d, 8), core)

    barrier = pltpu.get_barrier_semaphore()

    def greet(target):
        pl.semaphore_signal(barrier, inc=1, device_id=target, device_id_type=MESH)

    for step in PAIR_STEPS:
        greet((pair_to(step), aux))
    for d in RING:
        greet(y_to(d))
    greet(at(lax.rem(xhi + 1, 2) * 2 + xlo, y, z, core))
    greet(at(lax.rem(xhi + 1, 2) * 2 + 1 - xlo, y, z, core))
    greet(partner)
    for dz in range(1, 8):
        greet(at(x, y, lax.rem(z + dz, 8), other))

    def remote(src, dst, send, recv, target):
        return pltpu.make_async_remote_copy(
            src_ref=src,
            dst_ref=dst,
            send_sem=send,
            recv_sem=recv,
            device_id=target,
            device_id_type=MESH,
        )

    def arrived(ref, sems, target):
        remote(ref, ref, sems.at[0], sems.at[1], target).wait_recv()

    def left(ref, sems, target):
        remote(ref, ref, sems.at[0], sems.at[1], target).wait_send()

    loads = [
        pltpu.make_async_copy(src, dst, l_sem.at[i])
        for i, (src, dst) in enumerate(
            [
                (panel_ref, pbuf),
                (amplitude_ref, inamp),
                (energy_in, energy_ref),
                (fock_in, fock_ref),
                (occ_in, occ_ref),
                (freq_in, freq_ref),
                (lmo_in, lmo_ref),
                (near_in, near_ref),
                (rank_in, rank_ref),
            ]
        )
    ]
    for load in loads:
        load.start()
    loads[1].wait()
    loads[8].wait()
    slot_row = lax.broadcasted_iota(jnp.int32, (16, 120), 0)
    slot_col = lax.broadcasted_iota(jnp.int32, (16, 120), 1)
    pick = ((slot_row < 15) & (slot_col == chip * 15 + slot_row)).astype(jnp.float32)
    pick16 = pick.astype(jnp.bfloat16)
    amp_ref[...] = jnp.zeros_like(amp_ref)
    for s in range(2):
        rows = jnp.dot(pick16, inamp[core, s], preferred_element_type=jnp.float32)
        amp_ref[:, s * 128 : s * 128 + 120] = rows.astype(jnp.bfloat16)
    abuf[chip, core, pair] = amp_ref[...]
    loads[0].wait()
    place_row = lax.broadcasted_iota(jnp.int32, (128, 120), 0)
    place_col = lax.broadcasted_iota(jnp.int32, (128, 120), 1)
    fill = lax.rem(place_row, 16)
    source = place_row // 16 * 15 + fill
    for c in range(2):
        keep = (fill < 15) & (source == place_col) & (place_col < rank_ref[c])
        place = keep.astype(jnp.float32).astype(jnp.bfloat16)
        for t in range(9):
            cols = pl.ds(t * 256, 256)
            moved = jnp.dot(place, pbuf[c, :, cols], preferred_element_type=jnp.float32)
            mt_ref[c, cols, :] = moved.astype(jnp.bfloat16).T
    pl.semaphore_wait(barrier, 28)

    spare_row = lax.broadcasted_iota(jnp.int32, (16, 128), 0)
    spare_col = lax.broadcasted_iota(jnp.int32, (16, 128), 1)
    last = lax.rem(spare_col, 16) == 15

    def spare(first):
        hit = last & (spare_col // 16 == spare_row - first)
        return hit.astype(jnp.float32).astype(jnp.bfloat16)

    def pack(p):
        row = pl.multiple_of(p * 144, 16)
        mw[p, :144] = mt_ref[0, pl.ds(row, 144), :]
        mw[p, 144:] = mt_ref[1, pl.ds(row, 128), :]
        tail = mt_ref[1, pl.ds(pl.multiple_of(row + 128, 16), 16), :]
        for half in range(2):
            lines = slice(half * 128, half * 128 + 128)
            placed = lax.dot_general(
                tail,
                spare(half * 8),
                (((0,), (0,)), ((), ())),
                preferred_element_type=jnp.float32,
            )
            mw[p, lines] = (mw[p, lines].astype(jnp.float32) + placed).astype(jnp.bfloat16)
        return mw.at[p]

    def unpack(p, h):
        taken = lax.dot_general(
            spare(0),
            mbuf[p, h, :256],
            (((1,), (1,)), ((), ())),
            preferred_element_type=jnp.float32,
        )
        nb[p, h, 0] = mbuf[p, h, :144]
        nb[p, h, 1, :128] = mbuf[p, h, 144:]
        nb[p, h, 1, 128:] = jnp.concatenate(
            [taken[:8, :128], taken[:8, 128:]], axis=0
        ).astype(jnp.bfloat16)

    for dz in (1, 7, 2, 6, 3, 5, 4):
        remote(amp_ref, abuf.at[chip, core, pair], a_sem.at[0], a_sem.at[1], z_to(dz)).start()

    def send_block(i):
        p = pair_to(PAIR_STEPS[i])
        remote(pack(p), mbuf.at[pair, core], m_send, m_recv.at[i], (p, aux)).start()

    for i in range(NEAR):
        send_block(i)
    remote(pack(pair), mbuf.at[pair, core], f_send, f_recv.at[15], partner).start()
    for load in loads[2:8]:
        load.wait()
    lane = lax.broadcasted_iota(jnp.int32, (1, 128), 1)
    near_row = jnp.zeros((1, 128), jnp.int32)
    weight_row = jnp.zeros((1, 128), jnp.float32)
    for c in range(2):
        l0, l1 = lmo_ref[0, 2 * pair + c], lmo_ref[1, 2 * pair + c]
        near = [near_ref[c, k] for k in range(8)]
        value = [fock_ref[l0, lmo_ref[0, n]] + fock_ref[l1, lmo_ref[1, n]] for n in near]
        for k in range(8):
            weight = value[k]
            for j in range(k + 1, 8):
                weight = weight + jnp.where(near[j] == near[k], value[j], 0.0)
            for j in range(k):
                weight = jnp.where(near[j] == near[k], 0.0, weight)
            here = lane == c * 8 + k
            near_row = jnp.where(here, near[k], near_row)
            weight_row = jnp.where(here, weight, weight_row)
    weight_row = weight_row.astype(jnp.bfloat16).astype(jnp.float32)
    nbr_ref[...] = near_row
    wgt_ref[...] = weight_row
    nbuf[pair] = near_row
    wbuf[pair] = weight_row
    for i, step in enumerate(PAIR_STEPS):
        to = (pair_to(step), aux)
        remote(nbr_ref, nbuf.at[pair], n_sem.at[0], n_sem.at[1], to).start()
        remote(wgt_ref, wbuf.at[pair], w_sem.at[0], w_sem.at[1], to).start()
    nb[pair, core] = mt_ref[:, pl.ds(pl.multiple_of(pair * 144, 16), 144), :]
    diag[...] = jnp.zeros_like(diag)
    own_row = lax.broadcasted_iota(jnp.int32, (8, 120), 0) + chip * 15 + core * 7
    own = (lax.broadcasted_iota(jnp.int32, (8, 120), 1) == own_row).astype(jnp.float32)
    for c in range(2):
        across = energy_ref[pl.ds(c, 1), :]
        down = jnp.sum(own * across, axis=1, keepdims=True)
        occ = occ_ref[lmo_ref[0, 2 * pair + c]] + occ_ref[lmo_ref[1, 2 * pair + c]]
        shift = down + across - occ
        for s in range(2):
            rows = jnp.dot(
                own.astype(jnp.bfloat16), inamp[c, s], preferred_element_type=jnp.float32
            )
            sign = 1.0 - 2.0 * s
            diag[c, s, :, :120] = (shift - sign * freq_ref[0]) * rows

    def relay_block(i):
        step = PAIR_STEPS[i]
        p = pair_from(step)
        block = mbuf.at[p, core]
        remote(block, block, m_send, m_recv.at[i], (p, aux)).wait_recv()
        remote(block, block, f_send, f_recv.at[i], partner).start()
        unpack(p, core)

    def relayed(i):
        p = pair if i == 15 else pair_from(PAIR_STEPS[i])
        block = mbuf.at[p, other]
        remote(block, block, f_send, f_recv.at[i], partner).wait_recv()
        unpack(p, other)
        for h in range(2):
            mtr[p, h] = nb[p, h, core].T
        return p

    def project(p):
        for c in range(2):
            matrix = abuf[:, c, p].reshape(128, 256)
            for h in range(2):
                block = jnp.dot(nb[p, h, c], matrix, preferred_element_type=jnp.float32)
                proj[2 * p + c, h] = block.astype(jnp.bfloat16).astype(jnp.float32)

    def column(xx):
        return abuf.at[y * 2 + xx // 2, core, pl.ds(lax.rem(xx, 2) * 8, 8)]

    def rows_of(yy, cc):
        return abuf.at[pl.ds(yy * 2, 2), cc]

    arrived(abuf.at[0, 0, pl.ds(0, 7)], a_sem, partner)
    for d in RING:
        remote(column(x), column(x), b_sem.at[0], b_sem.at[1], x_to(d)).start()
    for d in RING:
        remote(column(x), column(x), y_sem.at[0], y_sem.at[1], y_to(d)).start()
    for i in range(NEAR, 15):
        send_block(i)
    relayed(15)
    relay_block(0)
    relay_block(1)
    relayed(0)
    arrived(abuf.at[pl.ds(0, 3), 0, pl.ds(0, 8)], b_sem, partner)
    for e in RING:
        for d in RING:
            xx = lax.rem(x + e, 4)
            remote(column(xx), column(xx), y_sem.at[0], y_sem.at[1], y_to(d)).start()
    remote(rows_of(y, core), rows_of(y, core), d_sem.at[0], d_sem.at[1], partner).start()
    for i in range(2, EARLY):
        relay_block(i)
        relayed(i - 1)
    arrived(abuf.at[pl.ds(0, 6), 0], y_sem, partner)
    for d in RING:
        yy = lax.rem(y + d, 4)
        remote(rows_of(yy, core), rows_of(yy, core), d_sem.at[0], d_sem.at[1], partner).start()
    relayed(EARLY - 1)
    relay_block(EARLY)
    arrived(nbuf.at[pl.ds(0, 15)], n_sem, partner)
    arrived(wbuf.at[pl.ds(0, 15)], w_sem, partner)
    to_nsm = pltpu.make_async_copy(nbuf, nsm, l_sem.at[0])
    to_wsm = pltpu.make_async_copy(wbuf, wsm, l_sem.at[1])
    to_nsm.start()
    to_wsm.start()
    to_nsm.wait()
    to_wsm.wait()
    arrived(abuf.at[:, 0], d_sem, partner)
    project(pair)
    for i in range(EARLY):
        project(pair_from(PAIR_STEPS[i]))
    for i in range(EARLY, 15):
        if i + 1 < 15:
            relay_block(i + 1)
        project(relayed(i))

    def close(lo, zz):
        odd = lax.rem(zz, 2)
        target = (1 - odd) * lax.rem(8 - zz // 2, 8) + odd * ((zz + 1) // 2)
        p = lo * 8 + target
        for h in range(2):
            total = jnp.zeros((144, 256), jnp.float32)
            for k in range(8):
                n = nsm[p, 0, core * 8 + k]
                w = wsm[p, 0, core * 8 + k]
                total = total + w * proj[n, h]
            coll[lo, h] = total.astype(jnp.bfloat16)
        closed = jnp.dot(mtr[p, 0], coll[lo, 0], preferred_element_type=jnp.float32)
        closed = closed + jnp.dot(mtr[p, 1], coll[lo, 1], preferred_element_type=jnp.float32)
        closed = closed.astype(jnp.bfloat16).reshape(4, 2, 16, 256)
        q, j = zz // SPAN, lax.rem(zz, SPAN)
        sa[:, q, :, lo, j] = closed[:, :, :, :128]
        for hi in range(2):
            sb[hi, lo, q, :, j] = closed[:, hi, :, 128:]

    def close_both(zz, carry):
        close(0, zz)
        close(1, zz)
        return carry

    def span(q):
        return pl.ds(q * SPAN, SPAN)

    for q in range(GROUPS):
        lax.fori_loop(q * SPAN, (q + 1) * SPAN, close_both, 0)
        for i, d in enumerate(RING):
            yy, xx = lax.rem(y + d, 4), lax.rem(x + d, 4)
            remote(
                sa.at[yy, q],
                ra.at[i, q],
                r_send.at[0],
                r_recv.at[0, q],
                y_to(d),
            ).start()
            remote(
                sb.at[xx // 2, lax.rem(xx, 2), q],
                rb.at[i, q],
                r_send.at[1],
                r_recv.at[1, q],
                x_to(d),
            ).start()

    def first_sum(q):
        part = ra.at[:, q]
        remote(part, part, r_send.at[0], r_recv.at[0, q], partner).wait_recv()
        total = sa[y, q].astype(jnp.float32)
        for i in range(3):
            total = total + ra[i, q].astype(jnp.float32)
        ta[:, :, span(q)] = total.astype(jnp.bfloat16)
        for i, d in enumerate(RING):
            xx = lax.rem(x + d, 4)
            remote(
                ta.at[xx // 2, lax.rem(xx, 2), span(q)],
                ca.at[i, span(q)],
                t_send.at[0],
                t_recv.at[0, q],
                x_to(d),
            ).start()
        part = rb.at[:, q]
        remote(part, part, r_send.at[1], r_recv.at[1, q], partner).wait_recv()
        total = sb[xhi, xlo, q].astype(jnp.float32)
        for i in range(3):
            total = total + rb[i, q].astype(jnp.float32)
        tb[:, span(q)] = total.astype(jnp.bfloat16)
        for i, d in enumerate(RING):
            yy = lax.rem(y + d, 4)
            remote(
                tb.at[yy, span(q)],
                cb.at[i, span(q)],
                t_send.at[1],
                t_recv.at[1, q],
                y_to(d),
            ).start()

    def second_sum(q):
        part = ca.at[:, span(q)]
        remote(part, part, t_send.at[0], t_recv.at[0, q], partner).wait_recv()
        total = ta[xhi, xlo, span(q)].astype(jnp.float32)
        for i in range(3):
            total = total + ca[i, span(q)].astype(jnp.float32)
        vbuf[span(q), 0, 0] = total[:, :8].astype(jnp.bfloat16)
        vbuf[span(q), 1, 0] = total[:, 7:15].astype(jnp.bfloat16)
        part = cb.at[:, span(q)]
        remote(part, part, t_send.at[1], t_recv.at[1, q], partner).wait_recv()
        total = tb[y, span(q)].astype(jnp.float32)
        for i in range(3):
            total = total + cb[i, span(q)].astype(jnp.float32)
        vbuf[span(q), 0, 1] = total[:, :8].astype(jnp.bfloat16)
        vbuf[span(q), 1, 1] = total[:, 7:15].astype(jnp.bfloat16)
        for j in range(q * SPAN, (q + 1) * SPAN):
            zz = Z_ORDER[j]
            slot = lax.rem(zz - z + 8, 8) * 2 + core
            remote(
                vbuf.at[j, other], ubuf.at[slot], u_sem.at[0], u_sem.at[1], at(x, y, zz, other)
            ).start()

            @pl.when(zz == z)
            def _():
                ubuf[core] = vbuf[j, core]

            @pl.when(zz != z)
            def _():
                remote(
                    vbuf.at[j, core], ubuf.at[slot], u_sem.at[0], u_sem.at[1], at(x, y, zz, core)
                ).start()

    for q in range(GROUPS + LAG):
        if q < GROUPS:
            first_sum(q)
        if q >= LAG:
            second_sum(q - LAG)
    arrived(ubuf.at[pl.ds(0, 15)], u_sem, partner)
    for c in range(2):
        total = diag[c]
        for slot in range(8):
            total = total + ubuf[slot * 2 + c].astype(jnp.float32)
        for s in range(2):
            line = slice(2 * c + s, 2 * c + s + 1)
            for j in range(8):
                flat[line, j * 120 : j * 120 + 120] = total[s, j : j + 1, :120]
            whole = flat[line, :]
            out_ref[c, s : s + 1, :] = jnp.where(core == 0, whole[:, :900], whole[:, 60:960])
    left(abuf.at[0, 0, pl.ds(0, 7)], a_sem, partner)
    left(abuf.at[pl.ds(0, 3), 0, pl.ds(0, 8)], b_sem, partner)
    left(abuf.at[pl.ds(0, 6), 0], y_sem, partner)
    left(abuf.at[:, 0], d_sem, partner)
    left(nbuf.at[pl.ds(0, 15)], n_sem, partner)
    left(wbuf.at[pl.ds(0, 15)], w_sem, partner)
    left(ubuf.at[pl.ds(0, 15)], u_sem, partner)
    blocks = mbuf.at[pl.ds(0, 15), 0]
    remote(blocks, blocks, m_send, m_recv.at[0], partner).wait_send()
    blocks = mbuf.at[:, 0]
    remote(blocks, blocks, f_send, f_recv.at[0], partner).wait_send()
    for half, (one, two) in enumerate([(ra, ca), (rb, cb)]):
        remote(one, one, r_send.at[half], r_recv.at[half, 0], partner).wait_send()
        remote(two, two, t_send.at[half], t_recv.at[half, 0], partner).wait_send()


def coupled_rows(*operands):
    bf16, f32, i32 = jnp.bfloat16, jnp.float32, jnp.int32
    dma = pltpu.SemaphoreType.DMA
    vmem, hbm = pl.BlockSpec(memory_space=pltpu.VMEM), pl.BlockSpec(memory_space=pltpu.HBM)
    return pl.pallas_call(
        kernel,
        out_shape=jax.ShapeDtypeStruct((2, 2, 900), f32),
        in_specs=[hbm] * 9,
        out_specs=vmem,
        scratch_shapes=[
            pltpu.VMEM((2, 120, 2304), bf16),
            pltpu.VMEM((2, 2, 120, 120), bf16),
            pltpu.VMEM((2, 120), f32),
            pltpu.SMEM((64, 64), f32),
            pltpu.SMEM((64,), f32),
            pltpu.SMEM((1,), f32),
            pltpu.SMEM((2, 32), i32),
            pltpu.SMEM((2, 8), i32),
            pltpu.SMEM((2,), i32),
            pltpu.VMEM((2, 2304, 128), bf16),
            pltpu.VMEM((16, 256), bf16),
            pltpu.VMEM((1, 128), i32),
            pltpu.VMEM((1, 128), f32),
            pltpu.VMEM((2, 2, 8, 128), f32),
            pltpu.VMEM((4, 1024), f32),
            pltpu.VMEM((16, 272, 128), bf16),
            pltpu.VMEM((16, 2, 272, 128), bf16),
            pltpu.VMEM((16, 2, 2, 144, 128), bf16),
            pltpu.VMEM((8, 2, 16, 16, 256), bf16),
            pltpu.VMEM((16, 1, 128), i32),
            pltpu.VMEM((16, 1, 128), f32),
            pltpu.SMEM((16, 1, 128), i32),
            pltpu.SMEM((16, 1, 128), f32),
            pltpu.VMEM((32, 2, 144, 256), f32),
            pltpu.VMEM((16, 2, 128, 144), bf16),
            pltpu.VMEM((2, 2, 144, 256), bf16),
            pltpu.VMEM((4, GROUPS, 2, 2, SPAN, 16, 128), bf16),
            pltpu.VMEM((2, 2, GROUPS, 4, SPAN, 16, 128), bf16),
            pltpu.VMEM((3, GROUPS, 2, 2, SPAN, 16, 128), bf16),
            pltpu.VMEM((3, GROUPS, 4, SPAN, 16, 128), bf16),
            pltpu.VMEM((2, 2, 8, 16, 128), bf16),
            pltpu.VMEM((4, 8, 16, 128), bf16),
            pltpu.VMEM((3, 8, 16, 128), bf16),
            pltpu.VMEM((3, 8, 16, 128), bf16),
            pltpu.VMEM((8, 2, 2, 8, 128), bf16),
            pltpu.VMEM((16, 2, 8, 128), bf16),
            dma((9,)),
            dma((2,)),
            dma((2,)),
            dma((2,)),
            dma((2,)),
            dma,
            dma((15,)),
            dma,
            dma((16,)),
            dma((2,)),
            dma((2,)),
            dma((2,)),
            dma((2, GROUPS)),
            dma((2,)),
            dma((2, GROUPS)),
            dma((2,)),
        ],
        compiler_params=pltpu.CompilerParams(
            collective_id=0, has_side_effects=True, vmem_limit_bytes=28 << 20
        ),
        name="coupled_rows",
    )(*[o if o.size == 1 else pltpu.with_memory_space_constraint(o, pltpu.HBM) for o in operands])


def body(
    panels,
    amplitudes,
    drive,
    pno_energy,
    occ_energy,
    frequency,
    pair_lmo,
    neighbours,
    pno_ranks,
    fock_off,
):
    return drive + coupled_rows(
        panels,
        amplitudes,
        pno_energy,
        fock_off,
        occ_energy,
        frequency,
        pair_lmo.T,
        neighbours,
        pno_ranks,
    )


def solution(mesh):
    placed = (
        P("pair", None, "aux"),
        P("pair", None, None, None),
        P("pair", None, "aux"),
        P("pair", None),
        P(),
        P(),
        P(),
        P("pair", None),
        P("pair"),
        P(),
    )
    return jax.shard_map(
        body, mesh=mesh, in_specs=placed, out_specs=P("pair", None, "aux"), check_vma=False
    )
```

```python
import jax
import jax.numpy as jnp
from jax import lax
from jax.experimental import pallas as pl
from jax.experimental.pallas import tpu as pltpu
from jax.sharding import PartitionSpec as P

MESH = pl.DeviceIdType.MESH

PAIR_STEPS = [(0, dz) for dz in (1, 7, 2, 6, 3, 5, 4)]
PAIR_STEPS += [(1, dz) for dz in (0, 1, 7, 2, 6, 3, 5, 4)]
NEAR = 7
RING = (2, 1, 3)
GROUPS = 4
SPAN = 8 // GROUPS
EARLY = 10
LAG = 4
Z_ORDER = (0, 1, 7, 2, 6, 3, 5, 4)


def kernel(
    panel_ref,
    amplitude_ref,
    energy_in,
    fock_in,
    occ_in,
    freq_in,
    lmo_in,
    near_in,
    rank_in,
    out_ref,
    pbuf,
    inamp,
    energy_ref,
    fock_ref,
    occ_ref,
    freq_ref,
    lmo_ref,
    near_ref,
    rank_ref,
    mt_ref,
    amp_ref,
    nbr_ref,
    wgt_ref,
    diag,
    flat,
    mw,
    mbuf,
    nb,
    abuf,
    nbuf,
    wbuf,
    nsm,
    wsm,
    proj,
    mtr,
    coll,
    sa,
    sb,
    ra,
    rb,
    ta,
    tb,
    ca,
    cb,
    vbuf,
    ubuf,
    l_sem,
    a_sem,
    b_sem,
    y_sem,
    d_sem,
    m_send,
    m_recv,
    f_send,
    f_recv,
    n_sem,
    w_sem,
    r_send,
    r_recv,
    t_send,
    t_recv,
    u_sem,
):
    pair = lax.axis_index("pair")
    aux = lax.axis_index("aux")
    xlo, z = pair // 8, lax.rem(pair, 8)
    chip, core = aux // 2, lax.rem(aux, 2)
    y, xhi = chip // 2, lax.rem(chip, 2)
    x = xhi * 2 + xlo
    other = 1 - core

    def at(xx, yy, zz, cc):
        return (lax.rem(xx, 2) * 8 + zz, (yy * 2 + xx // 2) * 2 + cc)

    partner = at(x, y, z, other)

    def pair_to(step):
        dx, dz = step
        return lax.rem(xlo + dx, 2) * 8 + lax.rem(z + dz, 8)

    def pair_from(step):
        dx, dz = step
        return lax.rem(xlo + dx, 2) * 8 + lax.rem(z + 8 - dz, 8)

    def x_to(d):
        return at(lax.rem(x + d, 4), y, z, core)

    def y_to(d):
        return at(x, lax.rem(y + d, 4), z, core)

    def z_to(d):
        return at(x, y, lax.rem(z + d, 8), core)

    barrier = pltpu.get_barrier_semaphore()

    def greet(target):
        pl.semaphore_signal(barrier, inc=1, device_id=target, device_id_type=MESH)

    for step in PAIR_STEPS:
        greet((pair_to(step), aux))
    for d in RING:
        greet(y_to(d))
    greet(at(lax.rem(xhi + 1, 2) * 2 + xlo, y, z, core))
    greet(at(lax.rem(xhi + 1, 2) * 2 + 1 - xlo, y, z, core))
    greet(partner)
    for dz in range(1, 8):
        greet(at(x, y, lax.rem(z + dz, 8), other))

    def remote(src, dst, send, recv, target):
        return pltpu.make_async_remote_copy(
            src_ref=src,
            dst_ref=dst,
            send_sem=send,
            recv_sem=recv,
            device_id=target,
            device_id_type=MESH,
        )

    def arrived(ref, sems, target):
        remote(ref, ref, sems.at[0], sems.at[1], target).wait_recv()

    def left(ref, sems, target):
        remote(ref, ref, sems.at[0], sems.at[1], target).wait_send()

    loads = [
        pltpu.make_async_copy(src, dst, l_sem.at[i])
        for i, (src, dst) in enumerate(
            [
                (panel_ref, pbuf),
                (amplitude_ref, inamp),
                (energy_in, energy_ref),
                (fock_in, fock_ref),
                (occ_in, occ_ref),
                (freq_in, freq_ref),
                (lmo_in, lmo_ref),
                (near_in, near_ref),
                (rank_in, rank_ref),
            ]
        )
    ]
    for load in loads:
        load.start()
    loads[1].wait()
    loads[8].wait()
    slot_row = lax.broadcasted_iota(jnp.int32, (16, 120), 0)
    slot_col = lax.broadcasted_iota(jnp.int32, (16, 120), 1)
    pick = ((slot_row < 15) & (slot_col == chip * 15 + slot_row)).astype(jnp.float32)
    pick16 = pick.astype(jnp.bfloat16)
    amp_ref[...] = jnp.zeros_like(amp_ref)
    for s in range(2):
        rows = jnp.dot(pick16, inamp[core, s], preferred_element_type=jnp.float32)
        amp_ref[:, s * 128 : s * 128 + 120] = rows.astype(jnp.bfloat16)
    abuf[chip, core, pair] = amp_ref[...]
    loads[0].wait()
    place_row = lax.broadcasted_iota(jnp.int32, (128, 120), 0)
    place_col = lax.broadcasted_iota(jnp.int32, (128, 120), 1)
    fill = lax.rem(place_row, 16)
    source = place_row // 16 * 15 + fill
    for c in range(2):
        keep = (fill < 15) & (source == place_col) & (place_col < rank_ref[c])
        place = keep.astype(jnp.float32).astype(jnp.bfloat16)
        for t in range(9):
            cols = pl.ds(t * 256, 256)
            moved = jnp.dot(place, pbuf[c, :, cols], preferred_element_type=jnp.float32)
            mt_ref[c, cols, :] = moved.astype(jnp.bfloat16).T
    pl.semaphore_wait(barrier, 28)

    spare_row = lax.broadcasted_iota(jnp.int32, (16, 128), 0)
    spare_col = lax.broadcasted_iota(jnp.int32, (16, 128), 1)
    last = lax.rem(spare_col, 16) == 15

    def spare(first):
        hit = last & (spare_col // 16 == spare_row - first)
        return hit.astype(jnp.float32).astype(jnp.bfloat16)

    def pack(p):
        row = pl.multiple_of(p * 144, 16)
        mw[p, :144] = mt_ref[0, pl.ds(row, 144), :]
        mw[p, 144:] = mt_ref[1, pl.ds(row, 128), :]
        tail = mt_ref[1, pl.ds(pl.multiple_of(row + 128, 16), 16), :]
        for half in range(2):
            lines = slice(half * 128, half * 128 + 128)
            placed = lax.dot_general(
                tail,
                spare(half * 8),
                (((0,), (0,)), ((), ())),
                preferred_element_type=jnp.float32,
            )
            mw[p, lines] = (mw[p, lines].astype(jnp.float32) + placed).astype(jnp.bfloat16)
        return mw.at[p]

    def unpack(p, h):
        taken = lax.dot_general(
            spare(0),
            mbuf[p, h, :256],
            (((1,), (1,)), ((), ())),
            preferred_element_type=jnp.float32,
        )
        nb[p, h, 0] = mbuf[p, h, :144]
        nb[p, h, 1, :128] = mbuf[p, h, 144:]
        nb[p, h, 1, 128:] = jnp.concatenate(
            [taken[:8, :128], taken[:8, 128:]], axis=0
        ).astype(jnp.bfloat16)

    for dz in (1, 7, 2, 6, 3, 5, 4):
        remote(amp_ref, abuf.at[chip, core, pair], a_sem.at[0], a_sem.at[1], z_to(dz)).start()

    def send_block(i):
        p = pair_to(PAIR_STEPS[i])
        remote(pack(p), mbuf.at[pair, core], m_send, m_recv.at[i], (p, aux)).start()

    for i in range(NEAR):
        send_block(i)
    remote(pack(pair), mbuf.at[pair, core], f_send, f_recv.at[15], partner).start()
    for load in loads[2:8]:
        load.wait()
    lane = lax.broadcasted_iota(jnp.int32, (1, 128), 1)
    near_row = jnp.zeros((1, 128), jnp.int32)
    weight_row = jnp.zeros((1, 128), jnp.float32)
    for c in range(2):
        l0, l1 = lmo_ref[0, 2 * pair + c], lmo_ref[1, 2 * pair + c]
        near = [near_ref[c, k] for k in range(8)]
        value = [fock_ref[l0, lmo_ref[0, n]] + fock_ref[l1, lmo_ref[1, n]] for n in near]
        for k in range(8):
            weight = value[k]
            for j in range(k + 1, 8):
                weight = weight + jnp.where(near[j] == near[k], value[j], 0.0)
            for j in range(k):
                weight = jnp.where(near[j] == near[k], 0.0, weight)
            here = lane == c * 8 + k
            near_row = jnp.where(here, near[k], near_row)
            weight_row = jnp.where(here, weight, weight_row)
    weight_row = weight_row.astype(jnp.bfloat16).astype(jnp.float32)
    nbr_ref[...] = near_row
    wgt_ref[...] = weight_row
    nbuf[pair] = near_row
    wbuf[pair] = weight_row
    for i, step in enumerate(PAIR_STEPS):
        to = (pair_to(step), aux)
        remote(nbr_ref, nbuf.at[pair], n_sem.at[0], n_sem.at[1], to).start()
        remote(wgt_ref, wbuf.at[pair], w_sem.at[0], w_sem.at[1], to).start()
    nb[pair, core] = mt_ref[:, pl.ds(pl.multiple_of(pair * 144, 16), 144), :]
    diag[...] = jnp.zeros_like(diag)
    own_row = lax.broadcasted_iota(jnp.int32, (8, 120), 0) + chip * 15 + core * 7
    own = (lax.broadcasted_iota(jnp.int32, (8, 120), 1) == own_row).astype(jnp.float32)
    for c in range(2):
        across = energy_ref[pl.ds(c, 1), :]
        down = jnp.sum(own * across, axis=1, keepdims=True)
        occ = occ_ref[lmo_ref[0, 2 * pair + c]] + occ_ref[lmo_ref[1, 2 * pair + c]]
        shift = down + across - occ
        for s in range(2):
            rows = jnp.dot(
                own.astype(jnp.bfloat16), inamp[c, s], preferred_element_type=jnp.float32
            )
            sign = 1.0 - 2.0 * s
            diag[c, s, :, :120] = (shift - sign * freq_ref[0]) * rows

    def relay_block(i):
        step = PAIR_STEPS[i]
        p = pair_from(step)
        block = mbuf.at[p, core]
        remote(block, block, m_send, m_recv.at[i], (p, aux)).wait_recv()
        remote(block, block, f_send, f_recv.at[i], partner).start()
        unpack(p, core)

    def relayed(i):
        p = pair if i == 15 else pair_from(PAIR_STEPS[i])
        block = mbuf.at[p, other]
        remote(block, block, f_send, f_recv.at[i], partner).wait_recv()
        unpack(p, other)
        for h in range(2):
            mtr[p, h] = nb[p, h, core].T
        return p

    def project(p):
        for c in range(2):
            matrix = abuf[:, c, p].reshape(128, 256)
            for h in range(2):
                block = jnp.dot(nb[p, h, c], matrix, preferred_element_type=jnp.float32)
                proj[2 * p + c, h] = block.astype(jnp.bfloat16).astype(jnp.float32)

    def column(xx):
        return abuf.at[y * 2 + xx // 2, core, pl.ds(lax.rem(xx, 2) * 8, 8)]

    def rows_of(yy, cc):
        return abuf.at[pl.ds(yy * 2, 2), cc]

    arrived(abuf.at[0, 0, pl.ds(0, 7)], a_sem, partner)
    for d in RING:
        remote(column(x), column(x), b_sem.at[0], b_sem.at[1], x_to(d)).start()
    for d in RING:
        remote(column(x), column(x), y_sem.at[0], y_sem.at[1], y_to(d)).start()
    for i in range(NEAR, 15):
        send_block(i)
    relayed(15)
    relay_block(0)
    relay_block(1)
    relayed(0)
    arrived(abuf.at[pl.ds(0, 3), 0, pl.ds(0, 8)], b_sem, partner)
    for e in RING:
        for d in RING:
            xx = lax.rem(x + e, 4)
            remote(column(xx), column(xx), y_sem.at[0], y_sem.at[1], y_to(d)).start()
    remote(rows_of(y, core), rows_of(y, core), d_sem.at[0], d_sem.at[1], partner).start()
    for i in range(2, EARLY):
        relay_block(i)
        relayed(i - 1)
    arrived(abuf.at[pl.ds(0, 6), 0], y_sem, partner)
    for d in RING:
        yy = lax.rem(y + d, 4)
        remote(rows_of(yy, core), rows_of(yy, core), d_sem.at[0], d_sem.at[1], partner).start()
    relayed(EARLY - 1)
    relay_block(EARLY)
    arrived(nbuf.at[pl.ds(0, 15)], n_sem, partner)
    arrived(wbuf.at[pl.ds(0, 15)], w_sem, partner)
    to_nsm = pltpu.make_async_copy(nbuf, nsm, l_sem.at[0])
    to_wsm = pltpu.make_async_copy(wbuf, wsm, l_sem.at[1])
    to_nsm.start()
    to_wsm.start()
    to_nsm.wait()
    to_wsm.wait()
    arrived(abuf.at[:, 0], d_sem, partner)
    project(pair)
    for i in range(EARLY):
        project(pair_from(PAIR_STEPS[i]))
    for i in range(EARLY, 15):
        if i + 1 < 15:
            relay_block(i + 1)
        project(relayed(i))

    def close(lo, zz):
        odd = lax.rem(zz, 2)
        target = (1 - odd) * lax.rem(8 - zz // 2, 8) + odd * ((zz + 1) // 2)
        p = lo * 8 + target
        for h in range(2):
            total = jnp.zeros((144, 256), jnp.float32)
            for k in range(8):
                n = nsm[p, 0, core * 8 + k]
                w = wsm[p, 0, core * 8 + k]
                total = total + w * proj[n, h]
            coll[lo, h] = total.astype(jnp.bfloat16)
        closed = jnp.dot(mtr[p, 0], coll[lo, 0], preferred_element_type=jnp.float32)
        closed = closed + jnp.dot(mtr[p, 1], coll[lo, 1], preferred_element_type=jnp.float32)
        closed = closed.astype(jnp.bfloat16).reshape(4, 2, 16, 256)
        q, j = zz // SPAN, lax.rem(zz, SPAN)
        sa[:, q, :, lo, j] = closed[:, :, :, :128]
        for hi in range(2):
            sb[hi, lo, q, :, j] = closed[:, hi, :, 128:]

    def close_both(zz, carry):
        close(0, zz)
        close(1, zz)
        return carry

    def span(q):
        return pl.ds(q * SPAN, SPAN)

    for q in range(GROUPS):
        lax.fori_loop(q * SPAN, (q + 1) * SPAN, close_both, 0)
        for i, d in enumerate(RING):
            yy, xx = lax.rem(y + d, 4), lax.rem(x + d, 4)
            remote(
                sa.at[yy, q],
                ra.at[i, q],
                r_send.at[0],
                r_recv.at[0, q],
                y_to(d),
            ).start()
            remote(
                sb.at[xx // 2, lax.rem(xx, 2), q],
                rb.at[i, q],
                r_send.at[1],
                r_recv.at[1, q],
                x_to(d),
            ).start()

    def first_sum(q):
        part = ra.at[:, q]
        remote(part, part, r_send.at[0], r_recv.at[0, q], partner).wait_recv()
        total = sa[y, q].astype(jnp.float32)
        for i in range(3):
            total = total + ra[i, q].astype(jnp.float32)
        ta[:, :, span(q)] = total.astype(jnp.bfloat16)
        for i, d in enumerate(RING):
            xx = lax.rem(x + d, 4)
            remote(
                ta.at[xx // 2, lax.rem(xx, 2), span(q)],
                ca.at[i, span(q)],
                t_send.at[0],
                t_recv.at[0, q],
                x_to(d),
            ).start()
        part = rb.at[:, q]
        remote(part, part, r_send.at[1], r_recv.at[1, q], partner).wait_recv()
        total = sb[xhi, xlo, q].astype(jnp.float32)
        for i in range(3):
            total = total + rb[i, q].astype(jnp.float32)
        tb[:, span(q)] = total.astype(jnp.bfloat16)
        for i, d in enumerate(RING):
            yy = lax.rem(y + d, 4)
            remote(
                tb.at[yy, span(q)],
                cb.at[i, span(q)],
                t_send.at[1],
                t_recv.at[1, q],
                y_to(d),
            ).start()

    def second_sum(q):
        part = ca.at[:, span(q)]
        remote(part, part, t_send.at[0], t_recv.at[0, q], partner).wait_recv()
        total = ta[xhi, xlo, span(q)].astype(jnp.float32)
        for i in range(3):
            total = total + ca[i, span(q)].astype(jnp.float32)
        vbuf[span(q), 0, 0] = total[:, :8].astype(jnp.bfloat16)
        vbuf[span(q), 1, 0] = total[:, 7:15].astype(jnp.bfloat16)
        part = cb.at[:, span(q)]
        remote(part, part, t_send.at[1], t_recv.at[1, q], partner).wait_recv()
        total = tb[y, span(q)].astype(jnp.float32)
        for i in range(3):
            total = total + cb[i, span(q)].astype(jnp.float32)
        vbuf[span(q), 0, 1] = total[:, :8].astype(jnp.bfloat16)
        vbuf[span(q), 1, 1] = total[:, 7:15].astype(jnp.bfloat16)
        for j in range(q * SPAN, (q + 1) * SPAN):
            zz = Z_ORDER[j]
            slot = lax.rem(zz - z + 8, 8) * 2 + core
            remote(
                vbuf.at[j, other], ubuf.at[slot], u_sem.at[0], u_sem.at[1], at(x, y, zz, other)
            ).start()

            @pl.when(zz == z)
            def _():
                ubuf[core] = vbuf[j, core]

            @pl.when(zz != z)
            def _():
                remote(
                    vbuf.at[j, core], ubuf.at[slot], u_sem.at[0], u_sem.at[1], at(x, y, zz, core)
                ).start()

    for q in range(GROUPS + LAG):
        if q < GROUPS:
            first_sum(q)
        if q >= LAG:
            second_sum(q - LAG)
    arrived(ubuf.at[pl.ds(0, 15)], u_sem, partner)
    for c in range(2):
        total = diag[c]
        for slot in range(8):
            total = total + ubuf[slot * 2 + c].astype(jnp.float32)
        for s in range(2):
            line = slice(2 * c + s, 2 * c + s + 1)
            for j in range(8):
                flat[line, j * 120 : j * 120 + 120] = total[s, j : j + 1, :120]
            whole = flat[line, :]
            out_ref[c, s : s + 1, :] = jnp.where(core == 0, whole[:, :900], whole[:, 60:960])
    left(abuf.at[0, 0, pl.ds(0, 7)], a_sem, partner)
    left(abuf.at[pl.ds(0, 3), 0, pl.ds(0, 8)], b_sem, partner)
    left(abuf.at[pl.ds(0, 6), 0], y_sem, partner)
    left(abuf.at[:, 0], d_sem, partner)
    left(nbuf.at[pl.ds(0, 15)], n_sem, partner)
    left(wbuf.at[pl.ds(0, 15)], w_sem, partner)
    left(ubuf.at[pl.ds(0, 15)], u_sem, partner)
    blocks = mbuf.at[pl.ds(0, 15), 0]
    remote(blocks, blocks, m_send, m_recv.at[0], partner).wait_send()
    blocks = mbuf.at[:, 0]
    remote(blocks, blocks, f_send, f_recv.at[0], partner).wait_send()
    for half, (one, two) in enumerate([(ra, ca), (rb, cb)]):
        remote(one, one, r_send.at[half], r_recv.at[half, 0], partner).wait_send()
        remote(two, two, t_send.at[half], t_recv.at[half, 0], partner).wait_send()


def coupled_rows(*operands):
    bf16, f32, i32 = jnp.bfloat16, jnp.float32, jnp.int32
    dma = pltpu.SemaphoreType.DMA
    vmem, hbm = pl.BlockSpec(memory_space=pltpu.VMEM), pl.BlockSpec(memory_space=pltpu.HBM)
    return pl.pallas_call(
        kernel,
        out_shape=jax.ShapeDtypeStruct((2, 2, 900), f32),
        in_specs=[hbm] * 9,
        out_specs=vmem,
        scratch_shapes=[
            pltpu.VMEM((2, 120, 2304), bf16),
            pltpu.VMEM((2, 2, 120, 120), bf16),
            pltpu.VMEM((2, 120), f32),
            pltpu.SMEM((64, 64), f32),
            pltpu.SMEM((64,), f32),
            pltpu.SMEM((1,), f32),
            pltpu.SMEM((2, 32), i32),
            pltpu.SMEM((2, 8), i32),
            pltpu.SMEM((2,), i32),
            pltpu.VMEM((2, 2304, 128), bf16),
            pltpu.VMEM((16, 256), bf16),
            pltpu.VMEM((1, 128), i32),
            pltpu.VMEM((1, 128), f32),
            pltpu.VMEM((2, 2, 8, 128), f32),
            pltpu.VMEM((4, 1024), f32),
            pltpu.VMEM((16, 272, 128), bf16),
            pltpu.VMEM((16, 2, 272, 128), bf16),
            pltpu.VMEM((16, 2, 2, 144, 128), bf16),
            pltpu.VMEM((8, 2, 16, 16, 256), bf16),
            pltpu.VMEM((16, 1, 128), i32),
            pltpu.VMEM((16, 1, 128), f32),
            pltpu.SMEM((16, 1, 128), i32),
            pltpu.SMEM((16, 1, 128), f32),
            pltpu.VMEM((32, 2, 144, 256), f32),
            pltpu.VMEM((16, 2, 128, 144), bf16),
            pltpu.VMEM((2, 2, 144, 256), bf16),
            pltpu.VMEM((4, GROUPS, 2, 2, SPAN, 16, 128), bf16),
            pltpu.VMEM((2, 2, GROUPS, 4, SPAN, 16, 128), bf16),
            pltpu.VMEM((3, GROUPS, 2, 2, SPAN, 16, 128), bf16),
            pltpu.VMEM((3, GROUPS, 4, SPAN, 16, 128), bf16),
            pltpu.VMEM((2, 2, 8, 16, 128), bf16),
            pltpu.VMEM((4, 8, 16, 128), bf16),
            pltpu.VMEM((3, 8, 16, 128), bf16),
            pltpu.VMEM((3, 8, 16, 128), bf16),
            pltpu.VMEM((8, 2, 2, 8, 128), bf16),
            pltpu.VMEM((16, 2, 8, 128), bf16),
            dma((9,)),
            dma((2,)),
            dma((2,)),
            dma((2,)),
            dma((2,)),
            dma,
            dma((15,)),
            dma,
            dma((16,)),
            dma((2,)),
            dma((2,)),
            dma((2,)),
            dma((2, GROUPS)),
            dma((2,)),
            dma((2, GROUPS)),
            dma((2,)),
        ],
        compiler_params=pltpu.CompilerParams(
            collective_id=0, has_side_effects=True, vmem_limit_bytes=28 << 20
        ),
        name="coupled_rows",
    )(*[o if o.size == 1 else pltpu.with_memory_space_constraint(o, pltpu.HBM) for o in operands])


def body(
    panels,
    amplitudes,
    drive,
    pno_energy,
    occ_energy,
    frequency,
    pair_lmo,
    neighbours,
    pno_ranks,
    fock_off,
):
    return drive + coupled_rows(
        panels,
        amplitudes,
        pno_energy,
        fock_off,
        occ_energy,
        frequency,
        pair_lmo.T,
        neighbours,
        pno_ranks,
    )


def solution(mesh):
    placed = (
        P("pair", None, "aux"),
        P("pair", None, None, None),
        P("pair", None, "aux"),
        P("pair", None),
        P(),
        P(),
        P(),
        P("pair", None),
        P("pair"),
        P(),
    )
    return jax.shard_map(
        body, mesh=mesh, in_specs=placed, out_specs=P("pair", None, "aux"), check_vma=False
    )
```
